512 devices in a mesh: row: 32 (over z_hi, x, core), col: 16 (over y, z_lo).
Axes of the slice: x: 4, y: 8, z: 8 (z_hi: 4, z_lo: 2; z = z_hi * 2 + z_lo), core: 2. Of those that a mesh axis runs over, the one named last changes fastest.
Arguments:
- source_points: float32 [3, 131072], P(None, 'col'), may hold values from 0 to 1
- source_areas: float32 [131072], P('col'), may hold values from 0.02 to 0.2
- source_fill: int32 [512], P('col'), may hold values from 128 to 256
- target_points: float32 [3, 131072], P(None, 'row'), may hold values from 0 to 1
- target_fill: int32 [512], P('row'), may hold values from 128 to 256
- charges: bfloat16 [64, 131072], P('row', 'col'), may hold values from -6 to 6
- near_fill: int32 [32, 16], P('row', 'col'), may hold values from 32 to 256, as said below
- near_source: int32 [32, 4096], P('row', 'col'), may hold values from 0 to 31
- near_target: int32 [32, 4096], P('row', 'col'), may hold values from 0 to 15
- far_source: int32 [32, 1536], P('row', 'col'), may hold values from 0 to 31
- far_target: int32 [32, 1536], P('row', 'col'), may hold values from 0 to 15
- far_rank: int32 [32, 1536], P('row', 'col'), may hold values from 8 to 32
- left_basis: bfloat16 [32, 1536, 32, 256], P('row', 'col'), may hold values from -0.25 to 0.25
- right_basis: bfloat16 [32, 1536, 32, 256], P('row', 'col'), may hold values from -0.375 to 0.375
Outputs:
- potential: float32 [64, 131072], P('col', 'row')
The draws below stay inside these ranges and needn't reach their ends.
Inputs may be any that keep to these rules, and one draw needn't show every extreme that they name: `near_fill`: used slots are the first ones of a device; in every row some device uses all 256. `near_source`: index among the 32 source leaves of the device's column group. `near_target`: index among the 16 target leaves of the device's row group. `far_source`: index among the 32 source leaves of the device's column group. `far_target`: index among the 16 target leaves of the device's row group. `far_rank`: factor rows from the rank on are padding.
All inputs are finite; a program needn't handle non-finite values.
Results may differ from the reference program's by a relative error of at most 0.0029.
Values may be sent and summed in bfloat16 or wider, within the bound.
A program may use at most 64 MiB of HBM per device.

```python
import math
import jax
import jax.numpy as jnp
from jax import lax

LEAF = 256
RANK = 32
RHS = 64
RL = 16
NEAR_DEV = 256
ADM_DEV = 96
CL = 32
NS = 131072
NT = 131072
N_ROW = 32
N_COL = 16


def draw_near_fill(key, part):
    row_index = jnp.arange(N_ROW)[:, None]
    col_index = jnp.arange(N_COL)[None, :]
    crowded = col_index == row_index * N_COL // N_ROW
    sparse_fill = jax.random.randint(jax.random.fold_in(key, 11), (N_ROW, N_COL), NEAR_DEV // 8, NEAR_DEV // 4 + 1)
    return jnp.where(crowded, NEAR_DEV, sparse_fill).astype(jnp.int32)


def touch_ends(drawn, own_key, smallest, largest):
    longest = drawn.shape.index(max(drawn.shape))
    spots = []
    for shift in (0, 1):
        where = [jax.random.randint(jax.random.fold_in(own_key, axis), (), 0, length) for axis, length in enumerate(drawn.shape)]
        where[longest] = (where[longest] + shift) % drawn.shape[longest]
        spots.append(tuple(where))
    return drawn.at[spots[0]].set(smallest).at[spots[1]].set(largest)


def level_of(own_key, shape, shards, smallest, high):
    level = 1.0
    for dim, blocks in shards:
        draws = jax.random.uniform(jax.random.fold_in(jax.random.fold_in(own_key, 6), dim), (blocks,), jnp.float32, smallest / len(shards), high / len(shards))
        level = level * jnp.repeat(jnp.exp(draws), shape[dim] // blocks).reshape((-1,) + (1,) * (len(shape) - 1 - dim))
    return level


def gaussian(rng, extent, deviation, reach, cuts=(), held_as=jnp.bfloat16):
    result = jax.random.normal(rng, extent, jnp.float32) * deviation
    if len(cuts) > 0:
        result = level_of(rng, extent, cuts, -0.22, 0.18) * result
    return jnp.clip(result, min=-reach, max=reach).astype(held_as)


def setup_inputs(seed: int = 0) -> dict:
    arg_keys = jax.random.split(jax.random.key(seed), 15)
    source_points = jnp.clip(1.0 * jax.random.uniform(arg_keys[0], (3, NS), jnp.float32) ** level_of(arg_keys[0], (3, NS), ((1, 16),), -0.2, 0.2), 0.0, 1.0)
    source_areas = jnp.clip(jnp.exp(math.log(0.2) - 2.3025851 * jax.random.uniform(arg_keys[1], (NS,), jnp.float32) ** level_of(arg_keys[1], (NS,), ((0, 16),), -0.2, 0.2)), 0.02, 0.2)
    source_fill = touch_ends(jax.random.randint(arg_keys[2], (CL * N_COL,), LEAF // 2, LEAF + 1), jax.random.fold_in(arg_keys[2], 1), LEAF // 2, LEAF).astype(jnp.int32)
    target_points = jnp.clip(1.0 * jax.random.uniform(arg_keys[3], (3, NT), jnp.float32) ** level_of(arg_keys[3], (3, NT), ((1, 32),), -0.2, 0.2), 0.0, 1.0)
    target_fill = touch_ends(jax.random.randint(arg_keys[4], (RL * N_ROW,), LEAF // 2, LEAF + 1), jax.random.fold_in(arg_keys[4], 1), LEAF // 2, LEAF).astype(jnp.int32)
    charges = gaussian(arg_keys[5], (RHS, NS), 1.0, 6.0, ((0, 32), (1, 16)))
    near_fill = draw_near_fill(jax.random.fold_in(arg_keys[14], 71), 0)
    near_source = touch_ends(jax.random.randint(arg_keys[7], (N_ROW, N_COL * NEAR_DEV), 0, CL), jax.random.fold_in(arg_keys[7], 1), 0, CL - 1).astype(jnp.int32)
    near_target = touch_ends(jax.random.randint(arg_keys[8], (N_ROW, N_COL * NEAR_DEV), 0, RL), jax.random.fold_in(arg_keys[8], 1), 0, RL - 1).astype(jnp.int32)
    far_source = touch_ends(jax.random.randint(arg_keys[9], (N_ROW, N_COL * ADM_DEV), 0, CL), jax.random.fold_in(arg_keys[9], 1), 0, CL - 1).astype(jnp.int32)
    far_target = touch_ends(jax.random.randint(arg_keys[10], (N_ROW, N_COL * ADM_DEV), 0, RL), jax.random.fold_in(arg_keys[10], 1), 0, RL - 1).astype(jnp.int32)
    far_rank = touch_ends(jax.random.randint(arg_keys[11], (N_ROW, N_COL * ADM_DEV), RANK // 4, RANK + 1), jax.random.fold_in(arg_keys[11], 1), RANK // 4, RANK).astype(jnp.int32)
    left_basis = gaussian(arg_keys[12], (N_ROW, N_COL * ADM_DEV, RANK, LEAF), (16 * RANK) ** -0.5, 0.25, ((0, 32), (1, 16)))
    right_basis = gaussian(arg_keys[13], (N_ROW, N_COL * ADM_DEV, RANK, LEAF), LEAF ** -0.5, 0.375, ((0, 32), (1, 16)))
    return dict(source_points=source_points, source_areas=source_areas, source_fill=source_fill, target_points=target_points, target_fill=target_fill, charges=charges, near_fill=near_fill, near_source=near_source, near_target=near_target, far_source=far_source, far_target=far_target, far_rank=far_rank, left_basis=left_basis, right_basis=right_basis)


INV_FOUR_PI = 0.07957747154594767
SOFTENING_SQ = 0.0025

def kernel_block(target_block, geometry):
    dist_sq = (target_block[0][:, None, :] - geometry[0][:, :, None]) ** 2
    dist_sq = dist_sq + (target_block[1][:, None, :] - geometry[1][:, :, None]) ** 2
    dist_sq = dist_sq + (target_block[2][:, None, :] - geometry[2][:, :, None]) ** 2
    return geometry[3][:, :, None] * INV_FOUR_PI * lax.rsqrt(dist_sq + SOFTENING_SQ)

def reference(source_points, source_areas, source_fill, target_points, target_fill, charges, near_fill, near_source, near_target, far_source, far_target, far_rank, left_basis, right_basis):
    devices_all = N_ROW * N_COL
    source_live = jnp.arange(LEAF, dtype=jnp.int32)[None, :] < source_fill[:, None]
    charge_grid = jnp.where(source_live[None], charges.reshape(RHS, CL * N_COL, LEAF), jnp.zeros((), charges.dtype))
    geometry_grid = jnp.concatenate([source_points, source_areas[None, :]], 0).reshape(4, CL * N_COL, LEAF)
    target_grid = target_points.reshape(3, RL * N_ROW, LEAF)
    row_base = (jnp.arange(N_ROW, dtype=jnp.int32) * RL)[:, None, None]
    col_base = (jnp.arange(N_COL, dtype=jnp.int32) * CL)[None, :, None]
    near_src_all = (near_source.reshape(N_ROW, N_COL, NEAR_DEV) + col_base).reshape(devices_all, NEAR_DEV).astype(jnp.int32)
    near_tgt_all = (near_target.reshape(N_ROW, N_COL, NEAR_DEV) + row_base).reshape(devices_all, NEAR_DEV).astype(jnp.int32)
    near_alive = jnp.arange(NEAR_DEV, dtype=jnp.int32)[None, :] < near_fill.reshape(devices_all, 1)
    far_src_all = (far_source.reshape(N_ROW, N_COL, ADM_DEV) + col_base).reshape(devices_all, ADM_DEV).astype(jnp.int32)
    far_tgt_all = (far_target.reshape(N_ROW, N_COL, ADM_DEV) + row_base).reshape(devices_all, ADM_DEV).astype(jnp.int32)
    rank_all = far_rank.reshape(devices_all, ADM_DEV)
    left_all = left_basis.reshape(devices_all, ADM_DEV, RANK, LEAF)
    right_all = right_basis.reshape(devices_all, ADM_DEV, RANK, LEAF)
    potential = jnp.zeros((RHS, RL * N_ROW, LEAF), jnp.float32)

    def near_step(running, slot_data):
        source_ids, target_ids, alive_mask = slot_data
        charge_block = jnp.take(charge_grid, source_ids, axis=1).astype(jnp.float32)
        geometry_block = jnp.take(geometry_grid, source_ids, axis=1)
        target_block = jnp.take(target_grid, target_ids, axis=1)
        entries = jnp.where(alive_mask[:, None, None], kernel_block(target_block, geometry_block), 0.0).astype(jnp.bfloat16)
        entries = lax.optimization_barrier(entries).astype(jnp.float32)
        blocks = jnp.einsum('ebs,bst->bet', charge_block, entries, precision=lax.Precision.HIGHEST)
        return (running.at[:, target_ids].add(jnp.transpose(blocks, (1, 0, 2))), None)

    def far_step(running, slot_data):
        source_ids, target_ids, ranks, left_slots, right_slots = slot_data
        gathered = jnp.take(charge_grid, source_ids, axis=1).astype(jnp.float32)
        coefficients = jnp.einsum('eas,ars->aer', gathered, right_slots.astype(jnp.float32), precision=lax.Precision.HIGHEST)
        rank_mask = jnp.arange(RANK, dtype=jnp.int32)[None, :] < ranks[:, None]
        coefficients = jnp.where(rank_mask[:, None, :], coefficients, 0.0).astype(jnp.bfloat16)
        coefficients = lax.optimization_barrier(coefficients).astype(jnp.float32)
        blocks = jnp.einsum('aer,art->aet', coefficients, left_slots.astype(jnp.float32), precision=lax.Precision.HIGHEST)
        return (running.at[:, target_ids].add(jnp.transpose(blocks, (1, 0, 2))), None)
    potential, _ = lax.scan(near_step, potential, (near_src_all, near_tgt_all, near_alive))
    potential, _ = lax.scan(far_step, potential, (far_src_all, far_tgt_all, rank_all, left_all, right_all))
    target_live = jnp.arange(LEAF, dtype=jnp.int32)[None, :] < target_fill[:, None]
    potential = jnp.where(target_live[None], potential, 0.0)
    return potential.reshape(RHS, RL * N_ROW * LEAF)
```

```python
import jax
import jax.numpy as jnp
from jax import lax
from jax.experimental import pallas as pl
from jax.experimental.pallas import tpu as pltpu
from jax.sharding import PartitionSpec as P

INV_FOUR_PI = 0.07957747154594767
SOFTENING_SQ = 0.0025
MESH = pl.DeviceIdType.MESH

LEAF = 256
RANK = 32
RL = 16
CL = 32
NEAR = 256
FAR = 96
N_ROW = 32
N_COL = 16
RHS = 64
NS = CL * LEAF
NT = RL * LEAF
FEAT = 48
ZERO = RL
FAR_BASE = RL + NEAR - FAR
SUMS = RL + NEAR

ENTRY_UNROLL = 16
FAR_UNROLL = 8
NEAR_UNROLL = 16
LANES = 128
F32 = jnp.float32
BF16 = jnp.bfloat16


def split3(value):
    high = value.astype(BF16).astype(F32)
    rest = value - high
    middle = rest.astype(BF16).astype(F32)
    low = (rest - middle).astype(BF16).astype(F32)
    return high, middle, low


def kernel(
    near_prev,
    near_last,
    far_prev,
    far_last,
    near_source,
    near_target,
    far_source,
    far_rank,
    source_fill,
    target_fill,
    source_points,
    source_areas,
    target_points,
    charges,
    left_hbm,
    right_hbm,
    out,
    grid_raw,
    grid,
    entries,
    sums,
    source_feat,
    target_feat,
    scaled,
    weight,
    plain,
    left,
    right,
    outgoing,
    from_side,
    merged,
    from_along,
    own_sem,
    basis_sem,
    z_send,
    z_recv,
    x_send,
    x_recv,
    pair_send,
    pair_recv,
    side_send,
    side_recv,
    along_send,
    along_recv,
):
    row = lax.axis_index("row")
    col = lax.axis_index("col")
    core = lax.rem(row, 2)
    x = lax.rem(row // 2, 4)
    z = row // 8

    def row_of(zz, xx, kk):
        return (zz * 4 + xx) * 2 + kk

    def back(a, d):
        return lax.rem(a + 4 - d, 4)

    def ahead(a, d):
        return lax.rem(a + d, 4)

    own_copy = pltpu.make_async_copy(charges, grid_raw.at[row], own_sem)
    own_copy.start()
    left_copy = pltpu.make_async_copy(left_hbm.at[0], left, basis_sem.at[0])
    right_copy = pltpu.make_async_copy(right_hbm.at[0], right, basis_sem.at[1])
    left_copy.start()
    right_copy.start()

    barrier = pltpu.get_barrier_semaphore()
    partner = row_of(z, x, 1 - core)
    peers = [partner]
    peers += [row_of(ahead(z, d), x, core) for d in (1, 2, 3)]
    peers += [row_of(z, ahead(x, d), core) for d in (1, 2, 3)]
    for peer in peers:
        pl.semaphore_signal(barrier, inc=1, device_id=(peer, col), device_id_type=MESH)
    for d in range(1, N_COL):
        pl.semaphore_signal(
            barrier, inc=1, device_id=(row, lax.rem(col + d, N_COL)), device_id_type=MESH
        )
    pl.semaphore_wait(barrier, len(peers) + N_COL - 1)

    def send(source, slot, peer, send_sem, recv_sem):
        return pltpu.make_async_remote_copy(
            src_ref=source,
            dst_ref=grid_raw.at[slot],
            send_sem=send_sem,
            recv_sem=recv_sem,
            device_id=(peer, col),
            device_id_type=MESH,
        )

    def z_copy(dz):
        return send(
            charges, row, row_of(ahead(z, dz), x, core), z_send.at[dz - 1], z_recv.at[dz - 1]
        )

    def x_copy(dx, dz):
        slot = row_of(back(z, dz), x, core)
        source = charges if dz == 0 else grid_raw.at[slot]
        return send(
            source,
            slot,
            row_of(z, ahead(x, dx), core),
            x_send.at[dx - 1, dz],
            x_recv.at[dx - 1, dz],
        )

    def pair_copy(dz, dx):
        slot = row_of(back(z, dz), back(x, dx), core)
        source = charges if dz == 0 and dx == 0 else grid_raw.at[slot]
        return send(source, slot, partner, pair_send.at[dz, dx], pair_recv.at[dz, dx])

    started = []

    def go(copy):
        copy.start()
        started.append(copy)

    for dz in (2, 1, 3):
        go(z_copy(dz))
    for dx in (2, 1, 3):
        go(x_copy(dx, 0))
    go(pair_copy(0, 0))

    centred = source_points[...] - 0.5
    area = source_areas[...].reshape(1, NS) * INV_FOUR_PI
    weight[...] = 1.0 / (area * area)
    plain[0:3, :] = centred * -2.0
    plain[3:4, :] = jnp.ones((1, NS), F32)
    squares = centred * centred
    plain[4:5, :] = squares[0:1] + squares[1:2] + squares[2:3] + SOFTENING_SQ
    plain[5:8, :] = jnp.zeros((3, NS), F32)

    def source_leaf(s, carry):
        points = pl.ds(pl.multiple_of(s * LEAF, LEAF), LEAF)
        high, middle, low = split3(plain[:, points] * weight[:, points])
        stacked = jnp.concatenate([high, high, middle, middle, high, low], 0)
        source_feat[s] = stacked.T.astype(BF16)
        return carry

    lax.fori_loop(0, CL, source_leaf, 0)

    away = target_points[...] - 0.5
    scaled[0:3, :] = away
    squares = away * away
    scaled[3:4, :] = squares[0:1] + squares[1:2] + squares[2:3]
    scaled[4:5, :] = jnp.ones((1, NT), F32)
    scaled[5:8, :] = jnp.zeros((3, NT), F32)

    def target_leaf(t, carry):
        points = pl.ds(pl.multiple_of(t * LEAF, LEAF), LEAF)
        high, middle, low = split3(scaled[:, points])
        stacked = jnp.concatenate([high, middle, high, middle, low, high], 0)
        target_feat[t] = stacked.astype(BF16)
        return carry

    lax.fori_loop(0, RL, target_leaf, 0)

    def entry_step(step, carry):
        for u in range(ENTRY_UNROLL):
            k = step * ENTRY_UNROLL + u
            scaled_sq = jnp.dot(
                source_feat[near_source[0, k]],
                target_feat[near_target[0, k]],
                preferred_element_type=F32,
            )
            entries[k] = lax.rsqrt(scaled_sq).astype(BF16)
        return carry

    def some_entries(first, last):
        lax.fori_loop(first // ENTRY_UNROLL, last // ENTRY_UNROLL, entry_step, 0)

    def from_z(dz):
        z_copy(dz).wait_recv()
        for dx in (2, 1, 3):
            go(x_copy(dx, dz))
        go(pair_copy(dz, 0))

    def from_x(dx, dz):
        x_copy(dx, dz).wait_recv()
        go(pair_copy(dz, dx))

    some_entries(0, 48)
    from_z(1)
    from_z(3)
    some_entries(48, 80)
    from_z(2)
    for dx in (1, 3, 2):
        from_x(dx, 0)
    some_entries(80, 144)
    for dz in (1, 3):
        for dx in (1, 3, 2):
            from_x(dx, dz)
    some_entries(144, 224)
    for dx in (1, 3, 2):
        from_x(dx, 2)
    some_entries(224, NEAR)
    own_copy.wait()
    for dz in range(4):
        for dx in range(4):
            pair_copy(dz, dx).wait_recv()
    for copy in started:
        copy.wait_send()

    lane = lax.broadcasted_iota(jnp.int32, (RHS, LEAF), 1)

    def charge_leaf(s, carry):
        points = pl.ds(pl.multiple_of(s * LEAF, LEAF), LEAF)
        block = grid_raw[:, :, points].reshape(RHS, LEAF)
        grid[s] = jnp.where(lane < source_fill[s], block.astype(F32), 0.0).astype(BF16)
        return carry

    lax.fori_loop(0, CL, charge_leaf, 0)

    left_copy.wait()
    right_copy.wait()
    sums[ZERO] = jnp.zeros((RHS, LEAF), F32)
    rank_lane = lax.broadcasted_iota(jnp.int32, (RHS, RANK), 1)

    def far_step(step, carry):
        blocks = []
        for u in range(FAR_UNROLL):
            k = step * FAR_UNROLL + u
            coefficients = lax.dot_general(
                grid[far_source[0, k]],
                right[k],
                (((1,), (1,)), ((), ())),
                preferred_element_type=F32,
            )
            coefficients = jnp.where(rank_lane < far_rank[0, k], coefficients, 0.0)
            blocks.append(
                jnp.dot(coefficients.astype(BF16), left[k], preferred_element_type=F32)
            )
        for u in range(FAR_UNROLL):
            k = step * FAR_UNROLL + u
            sums[FAR_BASE + k] = blocks[u] + sums[far_prev[0, k]]
        return carry

    lax.fori_loop(0, FAR // FAR_UNROLL, far_step, 0)

    for t in range(RL):
        sums[t] = sums[far_last[0, t]]

    def near_step(step, carry):
        blocks = []
        for u in range(NEAR_UNROLL):
            k = step * NEAR_UNROLL + u
            blocks.append(
                jnp.dot(grid[near_source[0, k]], entries[k], preferred_element_type=F32)
            )
        for u in range(NEAR_UNROLL):
            k = step * NEAR_UNROLL + u
            sums[RL + k] = blocks[u] + sums[near_prev[0, k]]
        return carry

    lax.fori_loop(0, NEAR // NEAR_UNROLL, near_step, 0)

    def pack_target(t, carry):
        points = pl.ds(pl.multiple_of(t * LEAF, LEAF), LEAF)
        value = jnp.where(lane < target_fill[t], sums[near_last[0, t]], 0.0).astype(BF16)
        for c in range(N_COL):
            outgoing[c, :, points] = value[4 * c : 4 * c + 4]
        return carry

    lax.fori_loop(0, RL, pack_target, 0)

    along = col // 2
    side = lax.rem(col, 2)

    def owner(d, which):
        return lax.rem(along + d, 8) * 2 + which

    def side_copy(d):
        return pltpu.make_async_remote_copy(
            src_ref=outgoing.at[owner(d, 1 - side)],
            dst_ref=from_side.at[d],
            send_sem=side_send.at[d],
            recv_sem=side_recv.at[d],
            device_id=(row, owner(0, 1 - side)),
            device_id_type=MESH,
        )

    def along_copy(d):
        return pltpu.make_async_remote_copy(
            src_ref=merged.at[d],
            dst_ref=from_along.at[d - 1],
            send_sem=along_send.at[d - 1],
            recv_sem=along_recv.at[d - 1],
            device_id=(row, owner(d, side)),
            device_id_type=MESH,
        )

    order = (4, 3, 5, 2, 6, 1, 7)
    for d in order + (0,):
        side_copy(d).start()
    for d in order:
        side_copy(d).wait_recv()
        both = outgoing[owner(d, side)].astype(F32) + from_side[d].astype(F32)
        merged[d] = both.astype(BF16)
        along_copy(d).start()
    side_copy(0).wait_recv()
    for d in order:
        along_copy(d).wait_recv()

    def add_up(step, carry):
        points = pl.ds(pl.multiple_of(step * 512, 512), 512)
        total = outgoing[col, :, points].astype(F32) + from_side[0, :, points].astype(F32)
        for d in order:
            total = total + from_along[d - 1, :, points].astype(F32)
        out[:, points] = total
        return carry

    lax.fori_loop(0, NT // 512, add_up, 0)
    for d in order:
        along_copy(d).wait_send()
        side_copy(d).wait_send()
    side_copy(0).wait_send()


def chain_kernel(near_target, far_target, near_fill, near_prev, near_last, far_prev, far_last):
    def chains(target, count, place, empty):
        across = jnp.broadcast_to(target, (count, count))
        down = across.T
        at_down = lax.broadcasted_iota(jnp.int32, (count, count), 0)
        at_across = lax.broadcasted_iota(jnp.int32, (count, count), 1)
        hit = (across == down) & (at_down < at_across)
        prev = jnp.max(jnp.where(hit, at_down + place, -1), axis=0, keepdims=True)
        return jnp.maximum(prev, empty), down

    def latest(down, count, place, live, empty):
        slot = lax.broadcasted_iota(jnp.int32, (count, LANES), 0)
        leaf = lax.broadcasted_iota(jnp.int32, (count, LANES), 1)
        hit = (down[:, :LANES] == leaf) & (slot < live)
        last = jnp.max(jnp.where(hit, slot + place, -1), axis=0, keepdims=True)
        return jnp.maximum(last, empty)

    leaf = lax.broadcasted_iota(jnp.int32, (1, LANES), 1)
    prev, down = chains(near_target[...], NEAR, RL, near_target[...])
    near_prev[...] = prev
    near_last[...] = latest(down, NEAR, RL, near_fill[0, 0], jnp.minimum(leaf, RL - 1))
    far = jnp.concatenate([far_target[...], jnp.full((1, LANES - FAR), RL, jnp.int32)], 1)
    prev, down = chains(far, LANES, FAR_BASE, ZERO)
    far_prev[...] = prev
    far_last[...] = latest(down, LANES, FAR_BASE, FAR, ZERO)


def shards(
    source_points,
    source_areas,
    source_fill,
    target_points,
    target_fill,
    charges,
    near_fill,
    near_source,
    near_target,
    far_source,
    far_target,
    far_rank,
    left_basis,
    right_basis,
):
    smem = pl.BlockSpec(memory_space=pltpu.SMEM)
    vmem = pl.BlockSpec(memory_space=pltpu.VMEM)
    hbm = pl.BlockSpec(memory_space=pl.ANY)
    dma = pltpu.SemaphoreType.DMA
    chains = pl.pallas_call(
        chain_kernel,
        name="chains",
        out_shape=[
            jax.ShapeDtypeStruct((1, NEAR), jnp.int32),
            jax.ShapeDtypeStruct((1, LANES), jnp.int32),
            jax.ShapeDtypeStruct((1, LANES), jnp.int32),
            jax.ShapeDtypeStruct((1, LANES), jnp.int32),
        ],
        in_specs=[vmem, vmem, smem],
        out_specs=[vmem] * 4,
    )(near_target, far_target, near_fill)
    return pl.pallas_call(
        kernel,
        name="block_low_rank",
        out_shape=jax.ShapeDtypeStruct((RHS // N_COL, NT), F32),
        in_specs=[smem] * 10 + [vmem] * 4 + [hbm] * 2,
        out_specs=vmem,
        scratch_shapes=[
            pltpu.VMEM((N_ROW, RHS // N_ROW, NS), BF16),
            pltpu.VMEM((CL, RHS, LEAF), BF16),
            pltpu.VMEM((NEAR, LEAF, LEAF), BF16),
            pltpu.VMEM((SUMS, RHS, LEAF), F32),
            pltpu.VMEM((CL, LEAF, FEAT), BF16),
            pltpu.VMEM((RL, FEAT, LEAF), BF16),
            pltpu.VMEM((8, NT), F32),
            pltpu.VMEM((1, NS), F32),
            pltpu.VMEM((8, NS), F32),
            pltpu.VMEM((FAR, RANK, LEAF), BF16),
            pltpu.VMEM((FAR, RANK, LEAF), BF16),
            pltpu.VMEM((N_COL, RHS // N_COL, NT), BF16),
            pltpu.VMEM((8, RHS // N_COL, NT), BF16),
            pltpu.VMEM((8, RHS // N_COL, NT), BF16),
            pltpu.VMEM((7, RHS // N_COL, NT), BF16),
            dma(()),
            dma((2,)),
            dma((3,)),
            dma((3,)),
            dma((3, 4)),
            dma((3, 4)),
            dma((4, 4)),
            dma((4, 4)),
            dma((8,)),
            dma((8,)),
            dma((7,)),
            dma((7,)),
        ],
        compiler_params=pltpu.CompilerParams(
            collective_id=0, has_side_effects=True, vmem_limit_bytes=64 * 1024 * 1024 - 65536
        ),
    )(
        *chains,
        near_source,
        near_target,
        far_source,
        far_rank,
        source_fill,
        target_fill,
        source_points,
        source_areas,
        target_points,
        charges,
        left_basis,
        right_basis,
    )


def solution(mesh):
    placed = (
        P(None, "col"),
        P("col"),
        P("col"),
        P(None, "row"),
        P("row"),
        P("row", "col"),
        P("row", "col"),
        P("row", "col"),
        P("row", "col"),
        P("row", "col"),
        P("row", "col"),
        P("row", "col"),
        P("row", "col", None, None),
        P("row", "col", None, None),
    )
    return jax.shard_map(
        shards, mesh=mesh, in_specs=placed, out_specs=P("col", "row"), check_vma=False
    )
```

```python
import jax
import jax.numpy as jnp
from jax import lax
from jax.experimental import pallas as pl
from jax.experimental.pallas import tpu as pltpu
from jax.sharding import PartitionSpec as P

INV_FOUR_PI = 0.07957747154594767
SOFTENING_SQ = 0.0025
MESH = pl.DeviceIdType.MESH

LEAF = 256
RANK = 32
RL = 16
CL = 32
NEAR = 256
FAR = 96
N_ROW = 32
N_COL = 16
RHS = 64
NS = CL * LEAF
NT = RL * LEAF
FEAT = 48
ZERO = RL
FAR_BASE = RL + NEAR - FAR
SUMS = RL + NEAR

ENTRY_UNROLL = 32
FAR_UNROLL = 16
NEAR_UNROLL = 32
LANES = 128
F32 = jnp.float32
BF16 = jnp.bfloat16


def split3(value):
    high = value.astype(BF16).astype(F32)
    rest = value - high
    middle = rest.astype(BF16).astype(F32)
    low = (rest - middle).astype(BF16).astype(F32)
    return high, middle, low


def kernel(
    near_prev,
    near_last,
    far_prev,
    far_last,
    near_source,
    near_target,
    far_source,
    far_rank,
    source_fill,
    target_fill,
    source_points,
    source_areas,
    target_points,
    charges,
    left_hbm,
    right_hbm,
    out,
    grid_raw,
    grid,
    entries,
    sums,
    source_feat,
    target_feat,
    scaled,
    weight,
    plain,
    left,
    right,
    coefficients,
    outgoing,
    kept,
    from_side,
    merged,
    from_along,
    own_sem,
    basis_sem,
    z_send,
    z_recv,
    x_send,
    x_recv,
    pair_send,
    pair_recv,
    side_send,
    side_recv,
    along_send,
    along_recv,
):
    row = lax.axis_index("row")
    col = lax.axis_index("col")
    core = lax.rem(row, 2)
    x = lax.rem(row // 2, 4)
    z = row // 8

    def row_of(zz, xx, kk):
        return (zz * 4 + xx) * 2 + kk

    def back(a, d):
        return lax.rem(a + 4 - d, 4)

    def ahead(a, d):
        return lax.rem(a + d, 4)

    own_copy = pltpu.make_async_copy(charges, grid_raw.at[row], own_sem)
    own_copy.start()
    left_copy = pltpu.make_async_copy(left_hbm.at[0], left, basis_sem.at[0])
    right_copy = pltpu.make_async_copy(right_hbm.at[0], right, basis_sem.at[1])
    left_copy.start()
    right_copy.start()

    barrier = pltpu.get_barrier_semaphore()
    partner = row_of(z, x, 1 - core)
    peers = [partner]
    peers += [row_of(ahead(z, d), x, core) for d in (1, 2, 3)]
    peers += [row_of(z, ahead(x, d), core) for d in (1, 2, 3)]
    for peer in peers:
        pl.semaphore_signal(barrier, inc=1, device_id=(peer, col), device_id_type=MESH)
    for d in range(1, N_COL):
        pl.semaphore_signal(
            barrier, inc=1, device_id=(row, lax.rem(col + d, N_COL)), device_id_type=MESH
        )
    centred = source_points[...] - 0.5
    area = source_areas[...].reshape(1, NS) * INV_FOUR_PI
    weight[...] = 1.0 / (area * area)
    plain[0:3, :] = centred * -2.0
    plain[3:4, :] = jnp.ones((1, NS), F32)
    squares = centred * centred
    plain[4:5, :] = squares[0:1] + squares[1:2] + squares[2:3] + SOFTENING_SQ
    plain[5:8, :] = jnp.zeros((3, NS), F32)

    def source_leaf(s, carry):
        points = pl.ds(pl.multiple_of(s * LEAF, LEAF), LEAF)
        high, middle, low = split3(plain[:, points] * weight[:, points])
        stacked = jnp.concatenate([high, high, middle, middle, high, low], 0)
        source_feat[s] = stacked.T.astype(BF16)
        return carry

    lax.fori_loop(0, CL, source_leaf, 0)

    away = target_points[...] - 0.5
    scaled[0:3, :] = away
    squares = away * away
    scaled[3:4, :] = squares[0:1] + squares[1:2] + squares[2:3]
    scaled[4:5, :] = jnp.ones((1, NT), F32)
    scaled[5:8, :] = jnp.zeros((3, NT), F32)

    def target_leaf(t, carry):
        points = pl.ds(pl.multiple_of(t * LEAF, LEAF), LEAF)
        high, middle, low = split3(scaled[:, points])
        stacked = jnp.concatenate([high, middle, high, middle, low, high], 0)
        target_feat[t] = stacked.astype(BF16)
        return carry

    lax.fori_loop(0, RL, target_leaf, 0)

    pl.semaphore_wait(barrier, len(peers) + N_COL - 1)

    def send(source, slot, peer, send_sem, recv_sem):
        return pltpu.make_async_remote_copy(
            src_ref=source,
            dst_ref=grid_raw.at[slot],
            send_sem=send_sem,
            recv_sem=recv_sem,
            device_id=(peer, col),
            device_id_type=MESH,
        )

    def z_copy(dz):
        return send(
            charges, row, row_of(ahead(z, dz), x, core), z_send.at[dz - 1], z_recv.at[dz - 1]
        )

    def x_copy(dx, dz):
        slot = row_of(back(z, dz), x, core)
        source = charges if dz == 0 else grid_raw.at[slot]
        return send(
            source,
            slot,
            row_of(z, ahead(x, dx), core),
            x_send.at[dx - 1, dz],
            x_recv.at[dx - 1, dz],
        )

    def pair_copy(dz, dx):
        slot = row_of(back(z, dz), back(x, dx), core)
        source = charges if dz == 0 and dx == 0 else grid_raw.at[slot]
        return send(source, slot, partner, pair_send.at[dz, dx], pair_recv.at[dz, dx])

    started = []

    def go(copy):
        copy.start()
        started.append(copy)

    for dz in (2, 1, 3):
        go(z_copy(dz))
    for dx in (2, 1, 3):
        go(x_copy(dx, 0))
    go(pair_copy(0, 0))

    def entry_step(step, carry):
        for u in range(ENTRY_UNROLL):
            k = step * ENTRY_UNROLL + u
            scaled_sq = jnp.dot(
                source_feat[near_source[0, k]],
                target_feat[near_target[0, k]],
                preferred_element_type=F32,
            )
            entries[k] = lax.rsqrt(scaled_sq).astype(BF16)
        return carry

    def some_entries(first, last):
        lax.fori_loop(first // ENTRY_UNROLL, last // ENTRY_UNROLL, entry_step, 0)

    def from_z(dz):
        z_copy(dz).wait_recv()
        for dx in (2, 1, 3):
            go(x_copy(dx, dz))
        go(pair_copy(dz, 0))

    def from_x(dx, dz):
        x_copy(dx, dz).wait_recv()
        go(pair_copy(dz, dx))

    some_entries(0, 64)
    from_z(1)
    from_z(3)
    some_entries(64, 96)
    from_z(2)
    for dx in (1, 3, 2):
        from_x(dx, 0)
    some_entries(96, 192)
    for dz in (1, 3):
        for dx in (1, 3, 2):
            from_x(dx, dz)
    some_entries(192, NEAR)
    for dx in (1, 3, 2):
        from_x(dx, 2)
    own_copy.wait()
    for dz in range(4):
        for dx in range(4):
            pair_copy(dz, dx).wait_recv()
    for copy in started:
        copy.wait_send()

    lane = lax.broadcasted_iota(jnp.int32, (RHS, LEAF), 1)

    def charge_leaf(s, carry):
        points = pl.ds(pl.multiple_of(s * LEAF, LEAF), LEAF)
        block = grid_raw[:, :, points].reshape(RHS, LEAF)
        grid[s] = jnp.where(lane < source_fill[s], block.astype(F32), 0.0).astype(BF16)
        return carry

    lax.fori_loop(0, CL, charge_leaf, 0)

    left_copy.wait()
    right_copy.wait()
    sums[ZERO] = jnp.zeros((RHS, LEAF), F32)
    rank_lane = lax.broadcasted_iota(jnp.int32, (RHS, RANK), 1)

    def far_coefficients(step):
        for u in range(FAR_UNROLL):
            k = step * FAR_UNROLL + u
            value = lax.dot_general(
                grid[far_source[0, k]],
                right[k],
                (((1,), (1,)), ((), ())),
                preferred_element_type=F32,
            )
            value = jnp.where(rank_lane < far_rank[0, k], value, 0.0)
            coefficients[k] = value.astype(BF16)

    def far_sums(step):
        blocks = []
        for u in range(FAR_UNROLL):
            k = step * FAR_UNROLL + u
            blocks.append(jnp.dot(coefficients[k], left[k], preferred_element_type=F32))
        for u in range(FAR_UNROLL):
            k = step * FAR_UNROLL + u
            sums[FAR_BASE + k] = blocks[u] + sums[far_prev[0, k]]

    def far_step(step, carry):
        far_sums(step)
        far_coefficients(step + 1)
        return carry

    far_coefficients(0)
    lax.fori_loop(0, FAR // FAR_UNROLL - 1, far_step, 0)
    far_sums(FAR // FAR_UNROLL - 1)

    for t in range(RL):
        sums[t] = sums[far_last[0, t]]

    def near_step(step, carry):
        blocks = []
        for u in range(NEAR_UNROLL):
            k = step * NEAR_UNROLL + u
            blocks.append(
                jnp.dot(grid[near_source[0, k]], entries[k], preferred_element_type=F32)
            )
        for u in range(NEAR_UNROLL):
            k = step * NEAR_UNROLL + u
            sums[RL + k] = blocks[u] + sums[near_prev[0, k]]
        return carry

    lax.fori_loop(0, NEAR // NEAR_UNROLL, near_step, 0)

    along = col // 2
    side = lax.rem(col, 2)

    def pack_target(t, carry):
        points = pl.ds(pl.multiple_of(t * LEAF, LEAF), LEAF)
        value = jnp.where(lane < target_fill[t], sums[near_last[0, t]], 0.0)
        for c in range(N_COL // 2):
            first = value[8 * c : 8 * c + 4]
            second = value[8 * c + 4 : 8 * c + 8]
            kept[c, :, points] = jnp.where(side == 0, first, second)
            outgoing[c, :, points] = jnp.where(side == 0, second, first).astype(BF16)
        return carry

    lax.fori_loop(0, RL, pack_target, 0)

    def owner(d):
        return lax.rem(along + d, 8)

    def side_copy(d):
        return pltpu.make_async_remote_copy(
            src_ref=outgoing.at[owner(d)],
            dst_ref=from_side.at[d],
            send_sem=side_send.at[d],
            recv_sem=side_recv.at[d],
            device_id=(row, along * 2 + 1 - side),
            device_id_type=MESH,
        )

    def along_copy(d):
        return pltpu.make_async_remote_copy(
            src_ref=merged.at[d],
            dst_ref=from_along.at[d - 1],
            send_sem=along_send.at[d - 1],
            recv_sem=along_recv.at[d - 1],
            device_id=(row, owner(d) * 2 + side),
            device_id_type=MESH,
        )

    order = (4, 3, 5, 2, 6, 1, 7)
    for d in order + (0,):
        side_copy(d).start()
    for d in order:
        side_copy(d).wait_recv()
        both = kept[owner(d)] + from_side[d].astype(F32)
        merged[d] = both.astype(BF16)
        along_copy(d).start()
    side_copy(0).wait_recv()
    for d in order:
        along_copy(d).wait_recv()

    def add_up(step, carry):
        points = pl.ds(pl.multiple_of(step * 512, 512), 512)
        total = kept[along, :, points] + from_side[0, :, points].astype(F32)
        for d in order:
            total = total + from_along[d - 1, :, points].astype(F32)
        out[:, points] = total
        return carry

    lax.fori_loop(0, NT // 512, add_up, 0)
    for d in order:
        along_copy(d).wait_send()
        side_copy(d).wait_send()
    side_copy(0).wait_send()


def chain_kernel(near_target, far_target, near_fill, near_prev, near_last, far_prev, far_last):
    def chains(target, count, place, empty):
        across = jnp.broadcast_to(target, (count, count))
        down = across.T
        at_down = lax.broadcasted_iota(jnp.int32, (count, count), 0)
        at_across = lax.broadcasted_iota(jnp.int32, (count, count), 1)
        hit = (across == down) & (at_down < at_across)
        prev = jnp.max(jnp.where(hit, at_down + place, -1), axis=0, keepdims=True)
        return jnp.maximum(prev, empty), down

    def latest(down, count, place, live, empty):
        slot = lax.broadcasted_iota(jnp.int32, (count, LANES), 0)
        leaf = lax.broadcasted_iota(jnp.int32, (count, LANES), 1)
        hit = (down[:, :LANES] == leaf) & (slot < live)
        last = jnp.max(jnp.where(hit, slot + place, -1), axis=0, keepdims=True)
        return jnp.maximum(last, empty)

    leaf = lax.broadcasted_iota(jnp.int32, (1, LANES), 1)
    prev, down = chains(near_target[...], NEAR, RL, near_target[...])
    near_prev[...] = prev
    near_last[...] = latest(down, NEAR, RL, near_fill[0, 0], jnp.minimum(leaf, RL - 1))
    far = jnp.concatenate([far_target[...], jnp.full((1, LANES - FAR), RL, jnp.int32)], 1)
    prev, down = chains(far, LANES, FAR_BASE, ZERO)
    far_prev[...] = prev
    far_last[...] = latest(down, LANES, FAR_BASE, FAR, ZERO)


def shards(
    source_points,
    source_areas,
    source_fill,
    target_points,
    target_fill,
    charges,
    near_fill,
    near_source,
    near_target,
    far_source,
    far_target,
    far_rank,
    left_basis,
    right_basis,
):
    smem = pl.BlockSpec(memory_space=pltpu.SMEM)
    vmem = pl.BlockSpec(memory_space=pltpu.VMEM)
    hbm = pl.BlockSpec(memory_space=pl.ANY)
    dma = pltpu.SemaphoreType.DMA
    chains = pl.pallas_call(
        chain_kernel,
        name="chains",
        out_shape=[
            jax.ShapeDtypeStruct((1, NEAR), jnp.int32),
            jax.ShapeDtypeStruct((1, LANES), jnp.int32),
            jax.ShapeDtypeStruct((1, LANES), jnp.int32),
            jax.ShapeDtypeStruct((1, LANES), jnp.int32),
        ],
        in_specs=[vmem, vmem, smem],
        out_specs=[vmem] * 4,
    )(near_target, far_target, near_fill)
    return pl.pallas_call(
        kernel,
        name="block_low_rank",
        out_shape=jax.ShapeDtypeStruct((RHS // N_COL, NT), F32),
        in_specs=[smem] * 10 + [vmem] * 4 + [hbm] * 2,
        out_specs=vmem,
        scratch_shapes=[
            pltpu.VMEM((N_ROW, RHS // N_ROW, NS), BF16),
            pltpu.VMEM((CL, RHS, LEAF), BF16),
            pltpu.VMEM((NEAR, LEAF, LEAF), BF16),
            pltpu.VMEM((SUMS, RHS, LEAF), F32),
            pltpu.VMEM((CL, LEAF, FEAT), BF16),
            pltpu.VMEM((RL, FEAT, LEAF), BF16),
            pltpu.VMEM((8, NT), F32),
            pltpu.VMEM((1, NS), F32),
            pltpu.VMEM((8, NS), F32),
            pltpu.VMEM((FAR, RANK, LEAF), BF16),
            pltpu.VMEM((FAR, RANK, LEAF), BF16),
            pltpu.VMEM((FAR, RHS, RANK), BF16),
            pltpu.VMEM((N_COL // 2, RHS // N_COL, NT), BF16),
            pltpu.VMEM((N_COL // 2, RHS // N_COL, NT), F32),
            pltpu.VMEM((8, RHS // N_COL, NT), BF16),
            pltpu.VMEM((8, RHS // N_COL, NT), BF16),
            pltpu.VMEM((7, RHS // N_COL, NT), BF16),
            dma(()),
            dma((2,)),
            dma((3,)),
            dma((3,)),
            dma((3, 4)),
            dma((3, 4)),
            dma((4, 4)),
            dma((4, 4)),
            dma((8,)),
            dma((8,)),
            dma((7,)),
            dma((7,)),
        ],
        compiler_params=pltpu.CompilerParams(
            collective_id=0, has_side_effects=True, vmem_limit_bytes=64 * 1024 * 1024 - 65536
        ),
    )(
        *chains,
        near_source,
        near_target,
        far_source,
        far_rank,
        source_fill,
        target_fill,
        source_points,
        source_areas,
        target_points,
        charges,
        left_basis,
        right_basis,
    )


def solution(mesh):
    placed = (
        P(None, "col"),
        P("col"),
        P("col"),
        P(None, "row"),
        P("row"),
        P("row", "col"),
        P("row", "col"),
        P("row", "col"),
        P("row", "col"),
        P("row", "col"),
        P("row", "col"),
        P("row", "col"),
        P("row", "col", None, None),
        P("row", "col", None, None),
    )
    return jax.shard_map(
        shards, mesh=mesh, in_specs=placed, out_specs=P("col", "row"), check_vma=False
    )
```

```python
import jax
import jax.numpy as jnp
from jax import lax
from jax.experimental import pallas as pl
from jax.experimental.pallas import tpu as pltpu
from jax.sharding import PartitionSpec as P

INV_FOUR_PI = 0.07957747154594767
SOFTENING_SQ = 0.0025
MESH = pl.DeviceIdType.MESH

LEAF = 256
RANK = 32
RL = 16
CL = 32
NEAR = 256
FAR = 96
N_ROW = 32
N_COL = 16
RHS = 64
NS = CL * LEAF
NT = RL * LEAF
FEAT = 48
ZERO = RL
FAR_BASE = RL + NEAR - FAR
SUMS = RL + NEAR

ENTRY_UNROLL = 32
FAR_UNROLL = 16
NEAR_UNROLL = 32
LANES = 128
LEAF_UNROLL = 8
HALF = LEAF // 2
NT_HALF = NT // 2
F32 = jnp.float32
BF16 = jnp.bfloat16


def split3(value):
    high = value.astype(BF16).astype(F32)
    rest = value - high
    middle = rest.astype(BF16).astype(F32)
    low = (rest - middle).astype(BF16).astype(F32)
    return high, middle, low


def kernel(
    near_prev,
    near_last,
    far_prev,
    far_last,
    near_source,
    near_target,
    far_source,
    far_rank,
    source_fill,
    target_fill,
    source_points,
    source_areas,
    target_points,
    charges,
    left_hbm,
    right_hbm,
    out,
    grid_raw,
    grid,
    entries,
    sums,
    source_feat,
    target_feat,
    scaled,
    weight,
    plain,
    left,
    right,
    coefficients,
    outgoing,
    kept,
    from_side,
    merged,
    from_along,
    own_sem,
    basis_sem,
    z_send,
    z_recv,
    x_send,
    x_recv,
    pair_send,
    pair_recv,
    side_send,
    side_recv,
    along_send,
    along_recv,
):
    row = lax.axis_index("row")
    col = lax.axis_index("col")
    core = lax.rem(row, 2)
    x = lax.rem(row // 2, 4)
    z = row // 8

    def row_of(zz, xx, kk):
        return (zz * 4 + xx) * 2 + kk

    def back(a, d):
        return lax.rem(a + 4 - d, 4)

    def ahead(a, d):
        return lax.rem(a + d, 4)

    own_copy = pltpu.make_async_copy(charges, grid_raw.at[row], own_sem)
    own_copy.start()
    left_copy = pltpu.make_async_copy(left_hbm.at[0], left, basis_sem.at[0])
    right_copy = pltpu.make_async_copy(right_hbm.at[0], right, basis_sem.at[1])
    left_copy.start()
    right_copy.start()

    barrier = pltpu.get_barrier_semaphore()
    partner = row_of(z, x, 1 - core)
    peers = [partner]
    peers += [row_of(ahead(z, d), x, core) for d in (1, 2, 3)]
    peers += [row_of(z, ahead(x, d), core) for d in (1, 2, 3)]
    for peer in peers:
        pl.semaphore_signal(barrier, inc=1, device_id=(peer, col), device_id_type=MESH)
    for d in range(1, N_COL):
        pl.semaphore_signal(
            barrier, inc=1, device_id=(row, lax.rem(col + d, N_COL)), device_id_type=MESH
        )
    centred = source_points[...] - 0.5
    area = source_areas[...].reshape(1, NS) * INV_FOUR_PI
    weight[...] = 1.0 / (area * area)
    plain[0:3, :] = centred * -2.0
    plain[3:4, :] = jnp.ones((1, NS), F32)
    squares = centred * centred
    plain[4:5, :] = squares[0:1] + squares[1:2] + squares[2:3] + SOFTENING_SQ
    plain[5:8, :] = jnp.zeros((3, NS), F32)

    away = target_points[...] - 0.5
    scaled[0:3, :] = away
    squares = away * away
    scaled[3:4, :] = squares[0:1] + squares[1:2] + squares[2:3]
    scaled[4:5, :] = jnp.ones((1, NT), F32)
    scaled[5:8, :] = jnp.zeros((3, NT), F32)

    def target_leaves(step, carry):
        for u in range(LEAF_UNROLL):
            t = step * LEAF_UNROLL + u
            points = pl.ds(pl.multiple_of(t * LEAF, LEAF), LEAF)
            high, middle, low = split3(scaled[:, points])
            stacked = jnp.concatenate([high, middle, high, middle, low, high], 0)
            target_feat[t] = stacked.astype(BF16)
        return carry

    lax.fori_loop(0, RL // LEAF_UNROLL, target_leaves, 0)

    pl.semaphore_wait(barrier, len(peers) + N_COL - 1)

    def send(source, slot, peer, send_sem, recv_sem):
        return pltpu.make_async_remote_copy(
            src_ref=source,
            dst_ref=grid_raw.at[slot],
            send_sem=send_sem,
            recv_sem=recv_sem,
            device_id=(peer, col),
            device_id_type=MESH,
        )

    def z_copy(dz):
        return send(
            charges, row, row_of(ahead(z, dz), x, core), z_send.at[dz - 1], z_recv.at[dz - 1]
        )

    def x_copy(dx, dz):
        slot = row_of(back(z, dz), x, core)
        source = charges if dz == 0 else grid_raw.at[slot]
        return send(
            source,
            slot,
            row_of(z, ahead(x, dx), core),
            x_send.at[dx - 1, dz],
            x_recv.at[dx - 1, dz],
        )

    def pair_copy(dz, dx):
        slot = row_of(back(z, dz), back(x, dx), core)
        source = charges if dz == 0 and dx == 0 else grid_raw.at[slot]
        return send(source, slot, partner, pair_send.at[dz, dx], pair_recv.at[dz, dx])

    started = []

    def go(copy):
        copy.start()
        started.append(copy)

    for dz in (2, 1, 3):
        go(z_copy(dz))
    for dx in (2, 1, 3):
        go(x_copy(dx, 0))
    go(pair_copy(0, 0))

    def source_leaves(step, carry):
        for u in range(LEAF_UNROLL):
            s = step * LEAF_UNROLL + u
            points = pl.ds(pl.multiple_of(s * LEAF, LEAF), LEAF)
            high, middle, low = split3(plain[:, points] * weight[:, points])
            stacked = jnp.concatenate([high, high, middle, middle, high, low], 0)
            source_feat[s] = stacked.T.astype(BF16)
        return carry

    lax.fori_loop(0, CL // LEAF_UNROLL, source_leaves, 0)

    def entry_step(step, carry):
        for u in range(ENTRY_UNROLL):
            k = step * ENTRY_UNROLL + u
            scaled_sq = jnp.dot(
                source_feat[near_source[0, k]],
                target_feat[near_target[0, k]],
                preferred_element_type=F32,
            )
            entries[k] = lax.rsqrt(scaled_sq).astype(BF16)
        return carry

    def some_entries(first, last):
        lax.fori_loop(first // ENTRY_UNROLL, last // ENTRY_UNROLL, entry_step, 0)

    def from_z(dz):
        z_copy(dz).wait_recv()
        for dx in (2, 1, 3):
            go(x_copy(dx, dz))
        go(pair_copy(dz, 0))

    def from_x(dx, dz):
        x_copy(dx, dz).wait_recv()
        go(pair_copy(dz, dx))

    some_entries(0, 96)
    from_z(1)
    from_z(3)
    some_entries(96, 128)
    from_z(2)
    for dx in (1, 3, 2):
        from_x(dx, 0)
    some_entries(128, 224)
    for dz in (1, 3):
        for dx in (1, 3, 2):
            from_x(dx, dz)
    some_entries(224, NEAR)
    for dx in (1, 3, 2):
        from_x(dx, 2)
    own_copy.wait()
    for dz in range(4):
        for dx in range(4):
            pair_copy(dz, dx).wait_recv()
    for copy in started:
        copy.wait_send()

    lane = lax.broadcasted_iota(jnp.int32, (RHS, LEAF), 1)

    def charge_leaf(s, carry):
        points = pl.ds(pl.multiple_of(s * LEAF, LEAF), LEAF)
        block = grid_raw[:, :, points].reshape(RHS, LEAF)
        grid[s] = jnp.where(lane < source_fill[s], block.astype(F32), 0.0).astype(BF16)
        return carry

    lax.fori_loop(0, CL, charge_leaf, 0)

    left_copy.wait()
    right_copy.wait()
    sums[ZERO] = jnp.zeros((RHS, LEAF), F32)
    rank_lane = lax.broadcasted_iota(jnp.int32, (RHS, RANK), 1)

    def far_coefficients(step):
        for u in range(FAR_UNROLL):
            k = step * FAR_UNROLL + u
            value = lax.dot_general(
                grid[far_source[0, k]],
                right[k],
                (((1,), (1,)), ((), ())),
                preferred_element_type=F32,
            )
            value = jnp.where(rank_lane < far_rank[0, k], value, 0.0)
            coefficients[k] = value.astype(BF16)

    def far_sums(first, count, lanes):
        blocks = []
        for u in range(count):
            k = first + u
            blocks.append(
                jnp.dot(coefficients[k], left[k, :, lanes], preferred_element_type=F32)
            )
        for u in range(count):
            k = first + u
            sums[FAR_BASE + k, :, lanes] = blocks[u] + sums[far_prev[0, k], :, lanes]

    def near_half(lanes):
        for t in range(RL):
            sums[t, :, lanes] = sums[far_last[0, t], :, lanes]

        def near_step(step, carry):
            blocks = []
            for u in range(NEAR_UNROLL):
                k = step * NEAR_UNROLL + u
                blocks.append(
                    jnp.dot(
                        grid[near_source[0, k]],
                        entries[k, :, lanes],
                        preferred_element_type=F32,
                    )
                )
            for u in range(NEAR_UNROLL):
                k = step * NEAR_UNROLL + u
                sums[RL + k, :, lanes] = blocks[u] + sums[near_prev[0, k], :, lanes]
            return carry

        lax.fori_loop(0, NEAR // NEAR_UNROLL, near_step, 0)

    along = col // 2
    side = lax.rem(col, 2)
    half_lane = lax.broadcasted_iota(jnp.int32, (RHS, HALF), 1)

    def pack_half(half, lanes):
        def pack_target(t, carry):
            points = pl.ds(pl.multiple_of(t * HALF, HALF), HALF)
            live = half_lane + half * HALF < target_fill[t]
            value = jnp.where(live, sums[near_last[0, t], :, lanes], 0.0)
            for c in range(N_COL // 2):
                first = value[8 * c : 8 * c + 4]
                second = value[8 * c + 4 : 8 * c + 8]
                kept[half, c, :, points] = jnp.where(side == 0, first, second)
                outgoing[half, c, :, points] = jnp.where(side == 0, second, first).astype(BF16)
            return carry

        lax.fori_loop(0, RL, pack_target, 0)

    def owner(d):
        return lax.rem(along + d, 8)

    def side_copy(half, d):
        return pltpu.make_async_remote_copy(
            src_ref=outgoing.at[half, owner(d)],
            dst_ref=from_side.at[half, d],
            send_sem=side_send.at[half, d],
            recv_sem=side_recv.at[half, d],
            device_id=(row, along * 2 + 1 - side),
            device_id_type=MESH,
        )

    def along_copy(half, d):
        return pltpu.make_async_remote_copy(
            src_ref=merged.at[half, d],
            dst_ref=from_along.at[half, d - 1],
            send_sem=along_send.at[half, d - 1],
            recv_sem=along_recv.at[half, d - 1],
            device_id=(row, owner(d) * 2 + side),
            device_id_type=MESH,
        )

    order = (4, 3, 5, 2, 6, 1, 7)

    def merge_half(half):
        for d in order:
            side_copy(half, d).wait_recv()
            both = kept[half, owner(d)] + from_side[half, d].astype(F32)
            merged[half, d] = both.astype(BF16)
            along_copy(half, d).start()

    def far_step(step, carry):
        far_sums(step * FAR_UNROLL, FAR_UNROLL, pl.ds(0, HALF))
        far_coefficients(step + 1)
        return carry

    far_coefficients(0)
    lax.fori_loop(0, FAR // FAR_UNROLL - 1, far_step, 0)
    far_sums(FAR - FAR_UNROLL, FAR_UNROLL, pl.ds(0, HALF))
    near_half(pl.ds(0, HALF))
    pack_half(0, pl.ds(0, HALF))
    for d in order + (0,):
        side_copy(0, d).start()

    def far_second(step, carry):
        far_sums(step * NEAR_UNROLL, NEAR_UNROLL, pl.ds(HALF, HALF))
        return carry

    lax.fori_loop(0, FAR // NEAR_UNROLL, far_second, 0)
    near_half(pl.ds(HALF, HALF))
    pack_half(1, pl.ds(HALF, HALF))
    for d in order + (0,):
        side_copy(1, d).start()
    merge_half(0)
    merge_half(1)
    for half in range(2):
        side_copy(half, 0).wait_recv()
        for d in order:
            along_copy(half, d).wait_recv()

    def add_up(t, carry):
        for half in range(2):
            points = pl.ds(pl.multiple_of(t * HALF, HALF), HALF)
            total = kept[half, along, :, points] + from_side[half, 0, :, points].astype(F32)
            for d in order:
                total = total + from_along[half, d - 1, :, points].astype(F32)
            out[:, pl.ds(pl.multiple_of(t * LEAF + half * HALF, HALF), HALF)] = total
        return carry

    lax.fori_loop(0, RL, add_up, 0)
    for half in range(2):
        for d in order:
            along_copy(half, d).wait_send()
            side_copy(half, d).wait_send()
        side_copy(half, 0).wait_send()


def chain_kernel(near_target, far_target, near_fill, near_prev, near_last, far_prev, far_last):
    def chains(target, count, place, empty):
        across = jnp.broadcast_to(target, (count, count))
        down = across.T
        at_down = lax.broadcasted_iota(jnp.int32, (count, count), 0)
        at_across = lax.broadcasted_iota(jnp.int32, (count, count), 1)
        hit = (across == down) & (at_down < at_across)
        prev = jnp.max(jnp.where(hit, at_down + place, -1), axis=0, keepdims=True)
        return jnp.maximum(prev, empty), down

    def latest(down, count, place, live, empty):
        slot = lax.broadcasted_iota(jnp.int32, (count, LANES), 0)
        leaf = lax.broadcasted_iota(jnp.int32, (count, LANES), 1)
        hit = (down[:, :LANES] == leaf) & (slot < live)
        last = jnp.max(jnp.where(hit, slot + place, -1), axis=0, keepdims=True)
        return jnp.maximum(last, empty)

    leaf = lax.broadcasted_iota(jnp.int32, (1, LANES), 1)
    prev, down = chains(near_target[...], NEAR, RL, near_target[...])
    near_prev[...] = prev
    near_last[...] = latest(down, NEAR, RL, near_fill[0, 0], jnp.minimum(leaf, RL - 1))
    far = jnp.concatenate([far_target[...], jnp.full((1, LANES - FAR), RL, jnp.int32)], 1)
    prev, down = chains(far, LANES, FAR_BASE, ZERO)
    far_prev[...] = prev
    far_last[...] = latest(down, LANES, FAR_BASE, FAR, ZERO)


def shards(
    source_points,
    source_areas,
    source_fill,
    target_points,
    target_fill,
    charges,
    near_fill,
    near_source,
    near_target,
    far_source,
    far_target,
    far_rank,
    left_basis,
    right_basis,
):
    smem = pl.BlockSpec(memory_space=pltpu.SMEM)
    vmem = pl.BlockSpec(memory_space=pltpu.VMEM)
    hbm = pl.BlockSpec(memory_space=pl.ANY)
    dma = pltpu.SemaphoreType.DMA
    chains = pl.pallas_call(
        chain_kernel,
        name="chains",
        out_shape=[
            jax.ShapeDtypeStruct((1, NEAR), jnp.int32),
            jax.ShapeDtypeStruct((1, LANES), jnp.int32),
            jax.ShapeDtypeStruct((1, LANES), jnp.int32),
            jax.ShapeDtypeStruct((1, LANES), jnp.int32),
        ],
        in_specs=[vmem, vmem, smem],
        out_specs=[vmem] * 4,
    )(near_target, far_target, near_fill)
    return pl.pallas_call(
        kernel,
        name="block_low_rank",
        out_shape=jax.ShapeDtypeStruct((RHS // N_COL, NT), F32),
        in_specs=[smem] * 10 + [vmem] * 4 + [hbm] * 2,
        out_specs=vmem,
        scratch_shapes=[
            pltpu.VMEM((N_ROW, RHS // N_ROW, NS), BF16),
            pltpu.VMEM((CL, RHS, LEAF), BF16),
            pltpu.VMEM((NEAR, LEAF, LEAF), BF16),
            pltpu.VMEM((SUMS, RHS, LEAF), F32),
            pltpu.VMEM((CL, LEAF, FEAT), BF16),
            pltpu.VMEM((RL, FEAT, LEAF), BF16),
            pltpu.VMEM((8, NT), F32),
            pltpu.VMEM((1, NS), F32),
            pltpu.VMEM((8, NS), F32),
            pltpu.VMEM((FAR, RANK, LEAF), BF16),
            pltpu.VMEM((FAR, RANK, LEAF), BF16),
            pltpu.VMEM((FAR, RHS, RANK), BF16),
            pltpu.VMEM((2, 8, RHS // N_COL, NT_HALF), BF16),
            pltpu.VMEM((2, 8, RHS // N_COL, NT_HALF), F32),
            pltpu.VMEM((2, 8, RHS // N_COL, NT_HALF), BF16),
            pltpu.VMEM((2, 8, RHS // N_COL, NT_HALF), BF16),
            pltpu.VMEM((2, 7, RHS // N_COL, NT_HALF), BF16),
            dma(()),
            dma((2,)),
            dma((3,)),
            dma((3,)),
            dma((3, 4)),
            dma((3, 4)),
            dma((4, 4)),
            dma((4, 4)),
            dma((2, 8)),
            dma((2, 8)),
            dma((2, 7)),
            dma((2, 7)),
        ],
        compiler_params=pltpu.CompilerParams(
            collective_id=0, has_side_effects=True, vmem_limit_bytes=64 * 1024 * 1024 - 65536
        ),
    )(
        *chains,
        near_source,
        near_target,
        far_source,
        far_rank,
        source_fill,
        target_fill,
        source_points,
        source_areas,
        target_points,
        charges,
        left_basis,
        right_basis,
    )


def solution(mesh):
    placed = (
        P(None, "col"),
        P("col"),
        P("col"),
        P(None, "row"),
        P("row"),
        P("row", "col"),
        P("row", "col"),
        P("row", "col"),
        P("row", "col"),
        P("row", "col"),
        P("row", "col"),
        P("row", "col"),
        P("row", "col", None, None),
        P("row", "col", None, None),
    )
    return jax.shard_map(
        shards, mesh=mesh, in_specs=placed, out_specs=P("col", "row"), check_vma=False
    )
```

```python
import jax
import jax.numpy as jnp
from jax import lax
from jax.experimental import pallas as pl
from jax.experimental.pallas import tpu as pltpu
from jax.sharding import PartitionSpec as P

INV_FOUR_PI = 0.07957747154594767
SOFTENING_SQ = 0.0025
MESH = pl.DeviceIdType.MESH

LEAF = 256
RANK = 32
RL = 16
CL = 32
NEAR = 256
FAR = 96
N_ROW = 32
N_COL = 16
RHS = 64
NS = CL * LEAF
NT = RL * LEAF
FEAT = 48
ZERO = RL
FAR_BASE = RL + NEAR - FAR
SUMS = RL + NEAR

ENTRY_UNROLL = 32
FAR_UNROLL = 16
NEAR_UNROLL = 32
LANES = 128
LEAF_UNROLL = 8
HALF = LEAF // 2
NEAR_STEPS = NEAR // NEAR_UNROLL
NT_HALF = NT // 2
F32 = jnp.float32
BF16 = jnp.bfloat16


def split3(value):
    high = value.astype(BF16).astype(F32)
    rest = value - high
    middle = rest.astype(BF16).astype(F32)
    low = (rest - middle).astype(BF16).astype(F32)
    return high, middle, low


def chains(target, count, place, empty):
    across = jnp.broadcast_to(target, (count, count))
    down = across.T
    at_down = lax.broadcasted_iota(jnp.int32, (count, count), 0)
    at_across = lax.broadcasted_iota(jnp.int32, (count, count), 1)
    hit = (across == down) & (at_down < at_across)
    prev = jnp.max(jnp.where(hit, at_down + place, -1), axis=0, keepdims=True)
    return jnp.maximum(prev, empty), down


def latest(down, count, place, live, empty):
    slot = lax.broadcasted_iota(jnp.int32, (count, LANES), 0)
    leaf = lax.broadcasted_iota(jnp.int32, (count, LANES), 1)
    hit = (down[:, :LANES] == leaf) & (slot < live)
    last = jnp.max(jnp.where(hit, slot + place, -1), axis=0, keepdims=True)
    return jnp.maximum(last, empty)


def kernel(
    near_target_hbm,
    far_target_hbm,
    near_fill,
    near_source_hbm,
    far_source_hbm,
    far_rank_hbm,
    source_fill_hbm,
    target_fill_hbm,
    source_points_hbm,
    source_areas_hbm,
    target_points_hbm,
    charges_hbm,
    left_hbm,
    right_hbm,
    out,
    grid_raw,
    grid,
    entries,
    sums,
    source_feat,
    target_feat,
    scaled,
    weight,
    plain,
    left,
    right,
    coefficients,
    outgoing,
    kept,
    from_side,
    merged,
    from_along,
    source_points,
    source_areas,
    target_points,
    near_across,
    far_across,
    near_prev_row,
    near_last_row,
    far_prev_row,
    far_last_row,
    near_target,
    near_source,
    far_source,
    far_rank,
    source_fill,
    target_fill,
    near_prev,
    near_last,
    far_prev,
    far_last,
    local_sem,
    z_send,
    z_recv,
    x_send,
    x_recv,
    pair_send,
    pair_recv,
    side_send,
    side_recv,
    along_send,
    along_recv,
):
    row = lax.axis_index("row")
    col = lax.axis_index("col")
    core = lax.rem(row, 2)
    x = lax.rem(row // 2, 4)
    z = row // 8

    def row_of(zz, xx, kk):
        return (zz * 4 + xx) * 2 + kk

    def back(a, d):
        return lax.rem(a + 4 - d, 4)

    def ahead(a, d):
        return lax.rem(a + d, 4)

    barrier = pltpu.get_barrier_semaphore()
    partner = row_of(z, x, 1 - core)
    peers = [partner]
    peers += [row_of(ahead(z, d), x, core) for d in (1, 2, 3)]
    peers += [row_of(z, ahead(x, d), core) for d in (1, 2, 3)]
    for peer in peers:
        pl.semaphore_signal(barrier, inc=1, device_id=(peer, col), device_id_type=MESH)
    for d in range(1, N_COL):
        pl.semaphore_signal(
            barrier, inc=1, device_id=(row, lax.rem(col + d, N_COL)), device_id_type=MESH
        )
    local = []

    def fetch(source, target):
        copy = pltpu.make_async_copy(source, target, local_sem.at[len(local)])
        copy.start()
        local.append(copy)
        return copy

    own_copy = fetch(charges_hbm, grid_raw.at[row])
    charges = grid_raw.at[row]
    point_copies = [
        fetch(target_points_hbm, target_points),
        fetch(source_points_hbm, source_points),
        fetch(source_areas_hbm, source_areas),
    ]
    chain_copies = [
        fetch(near_target_hbm, near_across),
        fetch(far_target_hbm, far_across),
    ]
    index_copies = [
        fetch(near_source_hbm, near_source),
        fetch(near_target_hbm, near_target),
        fetch(far_source_hbm, far_source),
        fetch(far_rank_hbm, far_rank),
        fetch(source_fill_hbm, source_fill),
        fetch(target_fill_hbm, target_fill),
    ]
    left_copy = fetch(left_hbm.at[0], left)
    right_copy = fetch(right_hbm.at[0], right)
    for copy in chain_copies + point_copies:
        copy.wait()

    prev, down = chains(near_across[...], NEAR, RL, near_across[...])
    near_prev_row[...] = prev
    leaf_lane = lax.broadcasted_iota(jnp.int32, (1, LANES), 1)
    near_last_row[...] = latest(down, NEAR, RL, near_fill[0, 0], jnp.minimum(leaf_lane, RL - 1))
    padding = jnp.full((1, LANES - FAR), RL, jnp.int32)
    prev, down = chains(
        jnp.concatenate([far_across[...], padding], 1), LANES, FAR_BASE, ZERO
    )
    far_prev_row[...] = prev
    far_last_row[...] = latest(down, LANES, FAR_BASE, FAR, ZERO)

    centred = source_points[...] - 0.5
    area = source_areas[...].reshape(1, NS) * INV_FOUR_PI
    weight[...] = 1.0 / (area * area)
    plain[0:3, :] = centred * -2.0
    plain[3:4, :] = jnp.ones((1, NS), F32)
    squares = centred * centred
    plain[4:5, :] = squares[0:1] + squares[1:2] + squares[2:3] + SOFTENING_SQ
    plain[5:8, :] = jnp.zeros((3, NS), F32)

    away = target_points[...] - 0.5
    scaled[0:3, :] = away
    squares = away * away
    scaled[3:4, :] = squares[0:1] + squares[1:2] + squares[2:3]
    scaled[4:5, :] = jnp.ones((1, NT), F32)
    scaled[5:8, :] = jnp.zeros((3, NT), F32)

    def target_leaves(step, carry):
        for u in range(LEAF_UNROLL):
            t = step * LEAF_UNROLL + u
            points = pl.ds(pl.multiple_of(t * LEAF, LEAF), LEAF)
            high, middle, low = split3(scaled[:, points])
            stacked = jnp.concatenate([high, middle, high, middle, low, high], 0)
            target_feat[t] = stacked.astype(BF16)
        return carry

    lax.fori_loop(0, RL // LEAF_UNROLL, target_leaves, 0)

    own_copy.wait()
    pl.semaphore_wait(barrier, len(peers) + N_COL - 1)

    def send(source, slot, peer, send_sem, recv_sem):
        return pltpu.make_async_remote_copy(
            src_ref=source,
            dst_ref=grid_raw.at[slot],
            send_sem=send_sem,
            recv_sem=recv_sem,
            device_id=(peer, col),
            device_id_type=MESH,
        )

    def z_copy(dz):
        return send(
            charges, row, row_of(ahead(z, dz), x, core), z_send.at[dz - 1], z_recv.at[dz - 1]
        )

    def x_copy(dx, dz):
        slot = row_of(back(z, dz), x, core)
        source = charges if dz == 0 else grid_raw.at[slot]
        return send(
            source,
            slot,
            row_of(z, ahead(x, dx), core),
            x_send.at[dx - 1, dz],
            x_recv.at[dx - 1, dz],
        )

    def pair_copy(dz, dx):
        slot = row_of(back(z, dz), back(x, dx), core)
        source = charges if dz == 0 and dx == 0 else grid_raw.at[slot]
        return send(source, slot, partner, pair_send.at[dz, dx], pair_recv.at[dz, dx])

    started = []

    def go(copy):
        copy.start()
        started.append(copy)

    for dz in (2, 1, 3):
        go(z_copy(dz))
    for dx in (2, 1, 3):
        go(x_copy(dx, 0))
    go(pair_copy(0, 0))

    def source_leaves(step, carry):
        for u in range(LEAF_UNROLL):
            s = step * LEAF_UNROLL + u
            points = pl.ds(pl.multiple_of(s * LEAF, LEAF), LEAF)
            high, middle, low = split3(plain[:, points] * weight[:, points])
            stacked = jnp.concatenate([high, high, middle, middle, high, low], 0)
            source_feat[s] = stacked.T.astype(BF16)
        return carry

    lax.fori_loop(0, CL // LEAF_UNROLL, source_leaves, 0)

    table_copies = [
        fetch(near_prev_row, near_prev),
        fetch(near_last_row, near_last),
        fetch(far_prev_row, far_prev),
        fetch(far_last_row, far_last),
    ]
    for copy in index_copies:
        copy.wait()

    def entry_step(step, carry):
        for u in range(ENTRY_UNROLL):
            k = step * ENTRY_UNROLL + u
            scaled_sq = jnp.dot(
                source_feat[near_source[0, k]],
                target_feat[near_target[0, k]],
                preferred_element_type=F32,
            )
            entries[k] = lax.rsqrt(scaled_sq).astype(BF16)
        return carry

    def some_entries(first, last):
        lax.fori_loop(first // ENTRY_UNROLL, last // ENTRY_UNROLL, entry_step, 0)

    def from_z(dz):
        z_copy(dz).wait_recv()
        for dx in (2, 1, 3):
            go(x_copy(dx, dz))
        go(pair_copy(dz, 0))

    def from_x(dx, dz):
        x_copy(dx, dz).wait_recv()
        go(pair_copy(dz, dx))

    some_entries(0, 96)
    from_z(1)
    from_z(3)
    some_entries(96, 128)
    from_z(2)
    for dx in (1, 3, 2):
        from_x(dx, 0)
    some_entries(128, 224)
    for dz in (1, 3):
        for dx in (1, 3, 2):
            from_x(dx, dz)
    some_entries(224, NEAR)
    for dx in (1, 3, 2):
        from_x(dx, 2)
    for dz in range(4):
        for dx in range(4):
            pair_copy(dz, dx).wait_recv()
    lane = lax.broadcasted_iota(jnp.int32, (RHS, LEAF), 1)

    def charge_leaf(s, carry):
        points = pl.ds(pl.multiple_of(s * LEAF, LEAF), LEAF)
        block = grid_raw[:, :, points].reshape(RHS, LEAF)
        grid[s] = jnp.where(lane < source_fill[s], block.astype(F32), 0.0).astype(BF16)
        return carry

    lax.fori_loop(0, CL, charge_leaf, 0)

    left_copy.wait()
    right_copy.wait()
    for copy in table_copies:
        copy.wait()
    sums[ZERO] = jnp.zeros((RHS, LEAF), F32)
    rank_lane = lax.broadcasted_iota(jnp.int32, (RHS, RANK), 1)

    def far_coefficients(step):
        for u in range(FAR_UNROLL):
            k = step * FAR_UNROLL + u
            value = lax.dot_general(
                grid[far_source[0, k]],
                right[k],
                (((1,), (1,)), ((), ())),
                preferred_element_type=F32,
            )
            value = jnp.where(rank_lane < far_rank[0, k], value, 0.0)
            coefficients[k] = value.astype(BF16)

    def far_sums(first, count, lanes):
        blocks = []
        for u in range(count):
            k = first + u
            blocks.append(
                jnp.dot(coefficients[k], left[k, :, lanes], preferred_element_type=F32)
            )
        for u in range(count):
            k = first + u
            sums[FAR_BASE + k, :, lanes] = blocks[u] + sums[far_prev[0, k], :, lanes]

    def near_start(lanes):
        for t in range(RL):
            sums[t, :, lanes] = sums[far_last[0, t], :, lanes]

    def near_part(lanes, first, last):
        def near_step(step, carry):
            blocks = []
            for u in range(NEAR_UNROLL):
                k = step * NEAR_UNROLL + u
                blocks.append(
                    jnp.dot(
                        grid[near_source[0, k]],
                        entries[k, :, lanes],
                        preferred_element_type=F32,
                    )
                )
            for u in range(NEAR_UNROLL):
                k = step * NEAR_UNROLL + u
                sums[RL + k, :, lanes] = blocks[u] + sums[near_prev[0, k], :, lanes]
            return carry

        lax.fori_loop(first, last, near_step, 0)

    along = col // 2
    side = lax.rem(col, 2)
    half_lane = lax.broadcasted_iota(jnp.int32, (RHS, HALF), 1)

    def pack_half(half, lanes):
        def pack_target(t, carry):
            points = pl.ds(pl.multiple_of(t * HALF, HALF), HALF)
            live = half_lane + half * HALF < target_fill[t]
            value = jnp.where(live, sums[near_last[0, t], :, lanes], 0.0)
            for c in range(N_COL // 2):
                first = value[8 * c : 8 * c + 4]
                second = value[8 * c + 4 : 8 * c + 8]
                kept[half, c, :, points] = jnp.where(side == 0, first, second)
                outgoing[half, c, :, points] = jnp.where(side == 0, second, first).astype(BF16)
            return carry

        lax.fori_loop(0, RL, pack_target, 0)

    def owner(d):
        return lax.rem(along + d, 8)

    def side_copy(half, d):
        return pltpu.make_async_remote_copy(
            src_ref=outgoing.at[half, owner(d)],
            dst_ref=from_side.at[half, d],
            send_sem=side_send.at[half, d],
            recv_sem=side_recv.at[half, d],
            device_id=(row, along * 2 + 1 - side),
            device_id_type=MESH,
        )

    def along_copy(half, d):
        return pltpu.make_async_remote_copy(
            src_ref=merged.at[half, d],
            dst_ref=from_along.at[half, d - 1],
            send_sem=along_send.at[half, d - 1],
            recv_sem=along_recv.at[half, d - 1],
            device_id=(row, owner(d) * 2 + side),
            device_id_type=MESH,
        )

    order = (4, 3, 5, 2, 6, 1, 7)

    def merge_half(half, some):
        for d in some:
            side_copy(half, d).wait_recv()
            both = kept[half, owner(d)] + from_side[half, d].astype(F32)
            merged[half, d] = both.astype(BF16)
            along_copy(half, d).start()

    def far_step(step, carry):
        far_sums(step * FAR_UNROLL, FAR_UNROLL, pl.ds(0, HALF))
        far_coefficients(step + 1)
        return carry

    far_coefficients(0)
    lax.fori_loop(0, FAR // FAR_UNROLL - 1, far_step, 0)
    far_sums(FAR - FAR_UNROLL, FAR_UNROLL, pl.ds(0, HALF))
    near_start(pl.ds(0, HALF))
    near_part(pl.ds(0, HALF), 0, NEAR_STEPS)
    pack_half(0, pl.ds(0, HALF))
    for d in order + (0,):
        side_copy(0, d).start()

    def far_second(step, carry):
        far_sums(step * NEAR_UNROLL, NEAR_UNROLL, pl.ds(HALF, HALF))
        return carry

    lax.fori_loop(0, FAR // NEAR_UNROLL, far_second, 0)
    near_start(pl.ds(HALF, HALF))
    near_part(pl.ds(HALF, HALF), 0, NEAR_STEPS - 3)
    merge_half(0, order[0:1])
    near_part(pl.ds(HALF, HALF), NEAR_STEPS - 3, NEAR_STEPS - 2)
    merge_half(0, order[1:3])
    near_part(pl.ds(HALF, HALF), NEAR_STEPS - 2, NEAR_STEPS - 1)
    merge_half(0, order[3:5])
    near_part(pl.ds(HALF, HALF), NEAR_STEPS - 1, NEAR_STEPS)
    pack_half(1, pl.ds(HALF, HALF))
    for d in order + (0,):
        side_copy(1, d).start()
    merge_half(0, order[5:7])
    merge_half(1, order)
    for half in range(2):
        side_copy(half, 0).wait_recv()
        for d in order:
            along_copy(half, d).wait_recv()

    def add_up(t, carry):
        for half in range(2):
            points = pl.ds(pl.multiple_of(t * HALF, HALF), HALF)
            total = kept[half, along, :, points] + from_side[half, 0, :, points].astype(F32)
            for d in order:
                total = total + from_along[half, d - 1, :, points].astype(F32)
            out[:, pl.ds(pl.multiple_of(t * LEAF + half * HALF, HALF), HALF)] = total
        return carry

    lax.fori_loop(0, RL, add_up, 0)
    for half in range(2):
        for d in order:
            along_copy(half, d).wait_send()
            side_copy(half, d).wait_send()
        side_copy(half, 0).wait_send()
    for copy in started:
        copy.wait_send()


def shards(
    source_points,
    source_areas,
    source_fill,
    target_points,
    target_fill,
    charges,
    near_fill,
    near_source,
    near_target,
    far_source,
    far_target,
    far_rank,
    left_basis,
    right_basis,
):
    vmem = pl.BlockSpec(memory_space=pltpu.VMEM)
    hbm = pl.BlockSpec(memory_space=pl.ANY)
    dma = pltpu.SemaphoreType.DMA
    return pl.pallas_call(
        kernel,
        name="block_low_rank",
        out_shape=jax.ShapeDtypeStruct((RHS // N_COL, NT), F32),
        in_specs=[hbm] * 2 + [pl.BlockSpec(memory_space=pltpu.SMEM)] + [hbm] * 11,
        out_specs=vmem,
        scratch_shapes=[
            pltpu.VMEM((N_ROW, RHS // N_ROW, NS), BF16),
            pltpu.VMEM((CL, RHS, LEAF), BF16),
            pltpu.VMEM((NEAR, LEAF, LEAF), BF16),
            pltpu.VMEM((SUMS, RHS, LEAF), F32),
            pltpu.VMEM((CL, LEAF, FEAT), BF16),
            pltpu.VMEM((RL, FEAT, LEAF), BF16),
            pltpu.VMEM((8, NT), F32),
            pltpu.VMEM((1, NS), F32),
            pltpu.VMEM((8, NS), F32),
            pltpu.VMEM((FAR, RANK, LEAF), BF16),
            pltpu.VMEM((FAR, RANK, LEAF), BF16),
            pltpu.VMEM((FAR, RHS, RANK), BF16),
            pltpu.VMEM((2, 8, RHS // N_COL, NT_HALF), BF16),
            pltpu.VMEM((2, 8, RHS // N_COL, NT_HALF), F32),
            pltpu.VMEM((2, 8, RHS // N_COL, NT_HALF), BF16),
            pltpu.VMEM((2, 8, RHS // N_COL, NT_HALF), BF16),
            pltpu.VMEM((2, 7, RHS // N_COL, NT_HALF), BF16),
            pltpu.VMEM((3, NS), F32),
            pltpu.VMEM((NS,), F32),
            pltpu.VMEM((3, NT), F32),
            pltpu.VMEM((1, NEAR), jnp.int32),
            pltpu.VMEM((1, FAR), jnp.int32),
            pltpu.VMEM((1, NEAR), jnp.int32),
            pltpu.VMEM((1, LANES), jnp.int32),
            pltpu.VMEM((1, LANES), jnp.int32),
            pltpu.VMEM((1, LANES), jnp.int32),
            pltpu.SMEM((1, NEAR), jnp.int32),
            pltpu.SMEM((1, NEAR), jnp.int32),
            pltpu.SMEM((1, FAR), jnp.int32),
            pltpu.SMEM((1, FAR), jnp.int32),
            pltpu.SMEM((CL,), jnp.int32),
            pltpu.SMEM((RL,), jnp.int32),
            pltpu.SMEM((1, NEAR), jnp.int32),
            pltpu.SMEM((1, LANES), jnp.int32),
            pltpu.SMEM((1, LANES), jnp.int32),
            pltpu.SMEM((1, LANES), jnp.int32),
            dma((18,)),
            dma((3,)),
            dma((3,)),
            dma((3, 4)),
            dma((3, 4)),
            dma((4, 4)),
            dma((4, 4)),
            dma((2, 8)),
            dma((2, 8)),
            dma((2, 7)),
            dma((2, 7)),
        ],
        compiler_params=pltpu.CompilerParams(
            collective_id=0, has_side_effects=True, vmem_limit_bytes=64 * 1024 * 1024 - 65536
        ),
    )(
        near_target,
        far_target,
        near_fill,
        near_source,
        far_source,
        far_rank,
        source_fill,
        target_fill,
        source_points,
        source_areas,
        target_points,
        charges,
        left_basis,
        right_basis,
    )


def solution(mesh):
    placed = (
        P(None, "col"),
        P("col"),
        P("col"),
        P(None, "row"),
        P("row"),
        P("row", "col"),
        P("row", "col"),
        P("row", "col"),
        P("row", "col"),
        P("row", "col"),
        P("row", "col"),
        P("row", "col"),
        P("row", "col", None, None),
        P("row", "col", None, None),
    )
    return jax.shard_map(
        shards, mesh=mesh, in_specs=placed, out_specs=P("col", "row"), check_vma=False
    )
```

```python
import jax
import jax.numpy as jnp
from jax import lax
from jax.experimental import pallas as pl
from jax.experimental.pallas import tpu as pltpu
from jax.sharding import PartitionSpec as P

INV_FOUR_PI = 0.07957747154594767
SOFTENING_SQ = 0.0025
MESH = pl.DeviceIdType.MESH

LEAF = 256
RANK = 32
RL = 16
CL = 32
NEAR = 256
FAR = 96
N_ROW = 32
N_COL = 16
RHS = 64
NS = CL * LEAF
NT = RL * LEAF
FEAT = 48
ZERO = RL
FAR_BASE = RL + NEAR - FAR
SUMS = RL + NEAR

ENTRY_UNROLL = 32
FAR_UNROLL = 16
NEAR_UNROLL = 32
LANES = 128
LEAF_UNROLL = 8
HALF = LEAF // 2
NEAR_STEPS = NEAR // NEAR_UNROLL
NT_HALF = NT // 2
F32 = jnp.float32
BF16 = jnp.bfloat16


def split3(value):
    high = value.astype(BF16).astype(F32)
    rest = value - high
    middle = rest.astype(BF16).astype(F32)
    low = (rest - middle).astype(BF16).astype(F32)
    return high, middle, low


def chains(target, count, place, empty):
    across = jnp.broadcast_to(target, (count, count))
    down = across.T
    at_down = lax.broadcasted_iota(jnp.int32, (count, count), 0)
    at_across = lax.broadcasted_iota(jnp.int32, (count, count), 1)
    hit = (across == down) & (at_down < at_across)
    prev = jnp.max(jnp.where(hit, at_down + place, -1), axis=0, keepdims=True)
    return jnp.maximum(prev, empty), down


def latest(down, count, place, live, empty):
    slot = lax.broadcasted_iota(jnp.int32, (count, LANES), 0)
    leaf = lax.broadcasted_iota(jnp.int32, (count, LANES), 1)
    hit = (down[:, :LANES] == leaf) & (slot < live)
    last = jnp.max(jnp.where(hit, slot + place, -1), axis=0, keepdims=True)
    return jnp.maximum(last, empty)


def kernel(
    near_target_hbm,
    far_target_hbm,
    near_fill,
    near_source_hbm,
    far_source_hbm,
    far_rank_hbm,
    source_fill_hbm,
    target_fill_hbm,
    source_points_hbm,
    source_areas_hbm,
    target_points_hbm,
    charges_hbm,
    left_hbm,
    right_hbm,
    out,
    grid_raw,
    grid,
    entries,
    sums,
    source_feat,
    target_feat,
    scaled,
    weight,
    plain,
    left,
    right,
    coefficients,
    outgoing,
    kept,
    from_side,
    merged,
    from_along,
    source_points,
    source_areas,
    target_points,
    near_across,
    far_across,
    near_prev_row,
    near_last_row,
    far_prev_row,
    far_last_row,
    near_target,
    near_source,
    far_source,
    far_rank,
    source_fill,
    target_fill,
    near_prev,
    near_last,
    far_prev,
    far_last,
    local_sem,
    z_send,
    z_recv,
    x_send,
    x_recv,
    pair_send,
    pair_recv,
    side_send,
    side_recv,
    along_send,
    along_recv,
):
    row = lax.axis_index("row")
    col = lax.axis_index("col")
    core = lax.rem(row, 2)
    x = lax.rem(row // 2, 4)
    z = row // 8

    def row_of(zz, xx, kk):
        return (zz * 4 + xx) * 2 + kk

    def back(a, d):
        return lax.rem(a + 4 - d, 4)

    def ahead(a, d):
        return lax.rem(a + d, 4)

    barrier = pltpu.get_barrier_semaphore()
    partner = row_of(z, x, 1 - core)
    peers = [partner]
    peers += [row_of(ahead(z, d), x, core) for d in (1, 2, 3)]
    peers += [row_of(z, ahead(x, d), core) for d in (1, 2, 3)]
    for peer in peers:
        pl.semaphore_signal(barrier, inc=1, device_id=(peer, col), device_id_type=MESH)
    for d in range(1, N_COL):
        pl.semaphore_signal(
            barrier, inc=1, device_id=(row, lax.rem(col + d, N_COL)), device_id_type=MESH
        )
    local = []

    def fetch(source, target):
        copy = pltpu.make_async_copy(source, target, local_sem.at[len(local)])
        copy.start()
        local.append(copy)
        return copy

    own_copy = fetch(charges_hbm, grid_raw.at[row])
    charges = grid_raw.at[row]
    point_copies = [
        fetch(target_points_hbm, target_points),
        fetch(source_points_hbm, source_points),
        fetch(source_areas_hbm, source_areas),
    ]
    chain_copies = [
        fetch(near_target_hbm, near_across),
        fetch(far_target_hbm, far_across),
    ]
    index_copies = [
        fetch(near_source_hbm, near_source),
        fetch(near_target_hbm, near_target),
        fetch(far_source_hbm, far_source),
        fetch(far_rank_hbm, far_rank),
        fetch(source_fill_hbm, source_fill),
        fetch(target_fill_hbm, target_fill),
    ]
    left_copy = fetch(left_hbm.at[0], left)
    right_copy = fetch(right_hbm.at[0], right)
    for copy in point_copies:
        copy.wait()

    centred = source_points[...] - 0.5
    area = source_areas[...].reshape(1, NS) * INV_FOUR_PI
    weight[...] = 1.0 / (area * area)
    plain[0:3, :] = centred * -2.0
    plain[3:4, :] = jnp.ones((1, NS), F32)
    squares = centred * centred
    plain[4:5, :] = squares[0:1] + squares[1:2] + squares[2:3] + SOFTENING_SQ
    plain[5:8, :] = jnp.zeros((3, NS), F32)

    away = target_points[...] - 0.5
    scaled[0:3, :] = away
    squares = away * away
    scaled[3:4, :] = squares[0:1] + squares[1:2] + squares[2:3]
    scaled[4:5, :] = jnp.ones((1, NT), F32)
    scaled[5:8, :] = jnp.zeros((3, NT), F32)

    def target_leaves(step, carry):
        for u in range(LEAF_UNROLL):
            t = step * LEAF_UNROLL + u
            points = pl.ds(pl.multiple_of(t * LEAF, LEAF), LEAF)
            high, middle, low = split3(scaled[:, points])
            stacked = jnp.concatenate([high, middle, high, middle, low, high], 0)
            target_feat[t] = stacked.astype(BF16)
        return carry

    lax.fori_loop(0, RL // LEAF_UNROLL, target_leaves, 0)

    own_copy.wait()
    pl.semaphore_wait(barrier, len(peers) + N_COL - 1)

    def send(source, slot, peer, send_sem, recv_sem):
        return pltpu.make_async_remote_copy(
            src_ref=source,
            dst_ref=grid_raw.at[slot],
            send_sem=send_sem,
            recv_sem=recv_sem,
            device_id=(peer, col),
            device_id_type=MESH,
        )

    def z_copy(dz):
        return send(
            charges, row, row_of(ahead(z, dz), x, core), z_send.at[dz - 1], z_recv.at[dz - 1]
        )

    def x_copy(dx, dz):
        slot = row_of(back(z, dz), x, core)
        source = charges if dz == 0 else grid_raw.at[slot]
        return send(
            source,
            slot,
            row_of(z, ahead(x, dx), core),
            x_send.at[dx - 1, dz],
            x_recv.at[dx - 1, dz],
        )

    def pair_copy(dz, dx):
        slot = row_of(back(z, dz), back(x, dx), core)
        source = charges if dz == 0 and dx == 0 else grid_raw.at[slot]
        return send(source, slot, partner, pair_send.at[dz, dx], pair_recv.at[dz, dx])

    started = []

    def go(copy):
        copy.start()
        started.append(copy)

    for dz in (2, 1, 3):
        go(z_copy(dz))
    for dx in (2, 1, 3):
        go(x_copy(dx, 0))
    go(pair_copy(0, 0))

    for copy in chain_copies:
        copy.wait()
    prev, down = chains(near_across[...], NEAR, RL, near_across[...])
    near_prev_row[...] = prev
    leaf_lane = lax.broadcasted_iota(jnp.int32, (1, LANES), 1)
    near_last_row[...] = latest(down, NEAR, RL, near_fill[0, 0], jnp.minimum(leaf_lane, RL - 1))
    padding = jnp.full((1, LANES - FAR), RL, jnp.int32)
    prev, down = chains(
        jnp.concatenate([far_across[...], padding], 1), LANES, FAR_BASE, ZERO
    )
    far_prev_row[...] = prev
    far_last_row[...] = latest(down, LANES, FAR_BASE, FAR, ZERO)

    def source_leaves(step, carry):
        for u in range(LEAF_UNROLL):
            s = step * LEAF_UNROLL + u
            points = pl.ds(pl.multiple_of(s * LEAF, LEAF), LEAF)
            high, middle, low = split3(plain[:, points] * weight[:, points])
            stacked = jnp.concatenate([high, high, middle, middle, high, low], 0)
            source_feat[s] = stacked.T.astype(BF16)
        return carry

    lax.fori_loop(0, CL // LEAF_UNROLL, source_leaves, 0)

    table_copies = [
        fetch(near_prev_row, near_prev),
        fetch(near_last_row, near_last),
        fetch(far_prev_row, far_prev),
        fetch(far_last_row, far_last),
    ]
    for copy in index_copies:
        copy.wait()

    def entry_step(step, carry):
        for u in range(ENTRY_UNROLL):
            k = step * ENTRY_UNROLL + u
            scaled_sq = jnp.dot(
                source_feat[near_source[0, k]],
                target_feat[near_target[0, k]],
                preferred_element_type=F32,
            )
            entries[k] = lax.rsqrt(scaled_sq).astype(BF16)
        return carry

    def some_entries(first, last):
        lax.fori_loop(first // ENTRY_UNROLL, last // ENTRY_UNROLL, entry_step, 0)

    def from_z(dz):
        z_copy(dz).wait_recv()
        for dx in (2, 1, 3):
            go(x_copy(dx, dz))
        go(pair_copy(dz, 0))

    def from_x(dx, dz):
        x_copy(dx, dz).wait_recv()
        go(pair_copy(dz, dx))

    some_entries(0, 96)
    from_z(1)
    from_z(3)
    some_entries(96, 128)
    from_z(2)
    for dx in (1, 3, 2):
        from_x(dx, 0)
    some_entries(128, 224)
    for dz in (1, 3):
        for dx in (1, 3, 2):
            from_x(dx, dz)
    some_entries(224, NEAR)
    for dx in (1, 3, 2):
        from_x(dx, 2)
    for dz in range(4):
        for dx in range(4):
            pair_copy(dz, dx).wait_recv()
    lane = lax.broadcasted_iota(jnp.int32, (RHS, LEAF), 1)

    def charge_leaves(step, carry):
        for u in range(LEAF_UNROLL):
            s = step * LEAF_UNROLL + u
            points = pl.ds(pl.multiple_of(s * LEAF, LEAF), LEAF)
            block = grid_raw[:, :, points].reshape(RHS, LEAF).astype(F32)
            grid[s] = jnp.where(lane < source_fill[s], block, 0.0).astype(BF16)
        return carry

    lax.fori_loop(0, CL // LEAF_UNROLL, charge_leaves, 0)

    left_copy.wait()
    right_copy.wait()
    for copy in table_copies:
        copy.wait()
    sums[ZERO] = jnp.zeros((RHS, LEAF), F32)
    rank_lane = lax.broadcasted_iota(jnp.int32, (RHS, RANK), 1)

    def far_coefficients(step):
        for u in range(FAR_UNROLL):
            k = step * FAR_UNROLL + u
            value = lax.dot_general(
                grid[far_source[0, k]],
                right[k],
                (((1,), (1,)), ((), ())),
                preferred_element_type=F32,
            )
            value = jnp.where(rank_lane < far_rank[0, k], value, 0.0)
            coefficients[k] = value.astype(BF16)

    def far_sums(first, count, lanes):
        blocks = []
        for u in range(count):
            k = first + u
            blocks.append(
                jnp.dot(coefficients[k], left[k, :, lanes], preferred_element_type=F32)
            )
        for u in range(count):
            k = first + u
            sums[FAR_BASE + k, :, lanes] = blocks[u] + sums[far_prev[0, k], :, lanes]

    def near_start(lanes):
        for t in range(RL):
            sums[t, :, lanes] = sums[far_last[0, t], :, lanes]

    def near_part(lanes, first, last):
        def near_step(step, carry):
            blocks = []
            for u in range(NEAR_UNROLL):
                k = step * NEAR_UNROLL + u
                blocks.append(
                    jnp.dot(
                        grid[near_source[0, k]],
                        entries[k, :, lanes],
                        preferred_element_type=F32,
                    )
                )
            for u in range(NEAR_UNROLL):
                k = step * NEAR_UNROLL + u
                sums[RL + k, :, lanes] = blocks[u] + sums[near_prev[0, k], :, lanes]
            return carry

        lax.fori_loop(first, last, near_step, 0)

    along = col // 2
    side = lax.rem(col, 2)
    half_lane = lax.broadcasted_iota(jnp.int32, (RHS, HALF), 1)

    def pack_half(half, lanes):
        def pack_target(t, carry):
            points = pl.ds(pl.multiple_of(t * HALF, HALF), HALF)
            live = half_lane + half * HALF < target_fill[t]
            value = jnp.where(live, sums[near_last[0, t], :, lanes], 0.0)
            for c in range(N_COL // 2):
                first = value[8 * c : 8 * c + 4]
                second = value[8 * c + 4 : 8 * c + 8]
                kept[half, c, :, points] = jnp.where(side == 0, first, second)
                outgoing[half, c, :, points] = jnp.where(side == 0, second, first).astype(BF16)
            return carry

        lax.fori_loop(0, RL, pack_target, 0)

    def owner(d):
        return lax.rem(along + d, 8)

    def side_copy(half, d):
        return pltpu.make_async_remote_copy(
            src_ref=outgoing.at[half, owner(d)],
            dst_ref=from_side.at[half, d],
            send_sem=side_send.at[half, d],
            recv_sem=side_recv.at[half, d],
            device_id=(row, along * 2 + 1 - side),
            device_id_type=MESH,
        )

    def along_copy(half, d):
        return pltpu.make_async_remote_copy(
            src_ref=merged.at[half, d],
            dst_ref=from_along.at[half, d - 1],
            send_sem=along_send.at[half, d - 1],
            recv_sem=along_recv.at[half, d - 1],
            device_id=(row, owner(d) * 2 + side),
            device_id_type=MESH,
        )

    order = (4, 3, 5, 2, 6, 1, 7)

    def merge_half(half, some):
        for d in some:
            side_copy(half, d).wait_recv()
            both = kept[half, owner(d)] + from_side[half, d].astype(F32)
            merged[half, d] = both.astype(BF16)
            along_copy(half, d).start()

    def far_step(step, carry):
        far_sums(step * FAR_UNROLL, FAR_UNROLL, pl.ds(0, HALF))
        far_coefficients(step + 1)
        return carry

    far_coefficients(0)
    lax.fori_loop(0, FAR // FAR_UNROLL - 1, far_step, 0)
    far_sums(FAR - FAR_UNROLL, FAR_UNROLL, pl.ds(0, HALF))
    near_start(pl.ds(0, HALF))
    near_part(pl.ds(0, HALF), 0, NEAR_STEPS)
    pack_half(0, pl.ds(0, HALF))
    for d in order + (0,):
        side_copy(0, d).start()

    def far_second(step, carry):
        far_sums(step * NEAR_UNROLL, NEAR_UNROLL, pl.ds(HALF, HALF))
        return carry

    lax.fori_loop(0, FAR // NEAR_UNROLL, far_second, 0)
    near_start(pl.ds(HALF, HALF))
    near_part(pl.ds(HALF, HALF), 0, NEAR_STEPS - 3)
    merge_half(0, order[0:1])
    near_part(pl.ds(HALF, HALF), NEAR_STEPS - 3, NEAR_STEPS - 2)
    merge_half(0, order[1:3])
    near_part(pl.ds(HALF, HALF), NEAR_STEPS - 2, NEAR_STEPS - 1)
    merge_half(0, order[3:5])
    near_part(pl.ds(HALF, HALF), NEAR_STEPS - 1, NEAR_STEPS)
    pack_half(1, pl.ds(HALF, HALF))
    for d in order + (0,):
        side_copy(1, d).start()
    merge_half(0, order[5:7])
    merge_half(1, order)
    for half in range(2):
        side_copy(half, 0).wait_recv()
        for d in order:
            along_copy(half, d).wait_recv()

    def add_up(t, carry):
        for half in range(2):
            points = pl.ds(pl.multiple_of(t * HALF, HALF), HALF)
            total = kept[half, along, :, points] + from_side[half, 0, :, points].astype(F32)
            for d in order:
                total = total + from_along[half, d - 1, :, points].astype(F32)
            out[:, pl.ds(pl.multiple_of(t * LEAF + half * HALF, HALF), HALF)] = total
        return carry

    lax.fori_loop(0, RL, add_up, 0)
    for half in range(2):
        for d in order:
            along_copy(half, d).wait_send()
            side_copy(half, d).wait_send()
        side_copy(half, 0).wait_send()
    for copy in started:
        copy.wait_send()


def shards(
    source_points,
    source_areas,
    source_fill,
    target_points,
    target_fill,
    charges,
    near_fill,
    near_source,
    near_target,
    far_source,
    far_target,
    far_rank,
    left_basis,
    right_basis,
):
    vmem = pl.BlockSpec(memory_space=pltpu.VMEM)
    hbm = pl.BlockSpec(memory_space=pl.ANY)
    dma = pltpu.SemaphoreType.DMA
    return pl.pallas_call(
        kernel,
        name="block_low_rank",
        out_shape=jax.ShapeDtypeStruct((RHS // N_COL, NT), F32),
        in_specs=[hbm] * 2 + [pl.BlockSpec(memory_space=pltpu.SMEM)] + [hbm] * 11,
        out_specs=vmem,
        scratch_shapes=[
            pltpu.VMEM((N_ROW, RHS // N_ROW, NS), BF16),
            pltpu.VMEM((CL, RHS, LEAF), BF16),
            pltpu.VMEM((NEAR, LEAF, LEAF), BF16),
            pltpu.VMEM((SUMS, RHS, LEAF), F32),
            pltpu.VMEM((CL, LEAF, FEAT), BF16),
            pltpu.VMEM((RL, FEAT, LEAF), BF16),
            pltpu.VMEM((8, NT), F32),
            pltpu.VMEM((1, NS), F32),
            pltpu.VMEM((8, NS), F32),
            pltpu.VMEM((FAR, RANK, LEAF), BF16),
            pltpu.VMEM((FAR, RANK, LEAF), BF16),
            pltpu.VMEM((FAR, RHS, RANK), BF16),
            pltpu.VMEM((2, 8, RHS // N_COL, NT_HALF), BF16),
            pltpu.VMEM((2, 8, RHS // N_COL, NT_HALF), F32),
            pltpu.VMEM((2, 8, RHS // N_COL, NT_HALF), BF16),
            pltpu.VMEM((2, 8, RHS // N_COL, NT_HALF), BF16),
            pltpu.VMEM((2, 7, RHS // N_COL, NT_HALF), BF16),
            pltpu.VMEM((3, NS), F32),
            pltpu.VMEM((NS,), F32),
            pltpu.VMEM((3, NT), F32),
            pltpu.VMEM((1, NEAR), jnp.int32),
            pltpu.VMEM((1, FAR), jnp.int32),
            pltpu.VMEM((1, NEAR), jnp.int32),
            pltpu.VMEM((1, LANES), jnp.int32),
            pltpu.VMEM((1, LANES), jnp.int32),
            pltpu.VMEM((1, LANES), jnp.int32),
            pltpu.SMEM((1, NEAR), jnp.int32),
            pltpu.SMEM((1, NEAR), jnp.int32),
            pltpu.SMEM((1, FAR), jnp.int32),
            pltpu.SMEM((1, FAR), jnp.int32),
            pltpu.SMEM((CL,), jnp.int32),
            pltpu.SMEM((RL,), jnp.int32),
            pltpu.SMEM((1, NEAR), jnp.int32),
            pltpu.SMEM((1, LANES), jnp.int32),
            pltpu.SMEM((1, LANES), jnp.int32),
            pltpu.SMEM((1, LANES), jnp.int32),
            dma((18,)),
            dma((3,)),
            dma((3,)),
            dma((3, 4)),
            dma((3, 4)),
            dma((4, 4)),
            dma((4, 4)),
            dma((2, 8)),
            dma((2, 8)),
            dma((2, 7)),
            dma((2, 7)),
        ],
        compiler_params=pltpu.CompilerParams(
            collective_id=0, has_side_effects=True, vmem_limit_bytes=64 * 1024 * 1024 - 65536
        ),
    )(
        near_target,
        far_target,
        near_fill,
        near_source,
        far_source,
        far_rank,
        source_fill,
        target_fill,
        source_points,
        source_areas,
        target_points,
        charges,
        left_basis,
        right_basis,
    )


def solution(mesh):
    placed = (
        P(None, "col"),
        P("col"),
        P("col"),
        P(None, "row"),
        P("row"),
        P("row", "col"),
        P("row", "col"),
        P("row", "col"),
        P("row", "col"),
        P("row", "col"),
        P("row", "col"),
        P("row", "col"),
        P("row", "col", None, None),
        P("row", "col", None, None),
    )
    return jax.shard_map(
        shards, mesh=mesh, in_specs=placed, out_specs=P("col", "row"), check_vma=False
    )
```
